32 devices in a mesh: dom: 32 (over z, y, x, core).
Axes of the slice: x: 2, y: 2, z: 4, core: 2. Of those that a mesh axis runs over, the one named last changes fastest.
Arguments:
- features: bfloat16 [32768, 512], P('dom'), may hold values from -6 to 6
- embeddings: bfloat16 [32768, 128], P('dom'), may hold values from -6 to 6
- tile_values: bfloat16 [256, 4, 128, 128], P('dom'), may hold values from -4 to 4
- tile_columns: int32 [256, 4], P('dom'), may hold values from 0 to 11
- send_blocks: int32 [32, 2, 2], P('dom'), may hold values from 0 to 7
- send_count: int32 [32, 2], P('dom'), may hold values from 1 to 2, as said below
- hub_rows: int32 [64], P('dom'), may hold values from 0 to 1023, as said below
- hub_weight: bfloat16 [32768, 64], P('dom'), may hold values from -4 to 4
- degree: int32 [32768], P('dom'), may hold values from 16 to 64
Outputs:
- hop_features: bfloat16 [3, 32768, 512], P(None, 'dom')
- hop_embeddings: bfloat16 [3, 32768, 128], P(None, 'dom')
The draws below stay inside these ranges and needn't reach their ends.
Inputs may be any that keep to these rules, and one draw needn't show every extreme that they name: `send_count`: some partition sends 2 blocks to its right and some to its left. `hub_rows`: the 2 hub rows of each partition are distinct local row numbers.
All inputs are finite; a program needn't handle non-finite values.
Results may differ from the reference program's by a relative error of at most 0.012.
Values may be sent and summed in bfloat16 or wider, within the bound.
No kernel may reach another device: no remote copies, remote signals or barrier semaphores. Data moves between devices by JAX's collectives and lax.ppermute only.
A program may use at most 64 MiB of HBM per device.

```python
import jax
import jax.numpy as jnp
from jax import lax

F = 512
E = 128
TILE = 128
ROWS_DEV = 1024
K = 4
SEND_MOST = 2
HUB_DEV = 2
HOPS = 3
ROWS = 32768
BLOCKS = 256
HUBS = 64
N_DOM = 32


def draw_send_count(key, part):
    counts = jax.random.randint(key, (N_DOM, 2), 1, SEND_MOST + 1)
    counts = counts.at[0, 1].set(SEND_MOST)
    counts = counts.at[N_DOM - 1, 0].set(SEND_MOST)
    return counts.astype(jnp.int32)


def draw_hub_rows(key, part):

    def one_device(device_index):
        return jax.random.permutation(jax.random.fold_in(key, device_index), ROWS_DEV)[:HUB_DEV]
    chosen = jax.vmap(one_device)(jnp.arange(N_DOM, dtype=jnp.int32))
    return chosen.reshape(-1).astype(jnp.int32)


def plant(array, stream_key, least, high):
    spot = [jax.random.randint(jax.random.fold_in(stream_key, axis), (), 0, length) for axis, length in enumerate(array.shape)]
    longest = array.shape.index(max(array.shape))
    next_to = spot[:longest] + [(spot[longest] + 1) % array.shape[longest]] + spot[longest + 1:]
    return array.at[tuple(spot)].set(least).at[tuple(next_to)].set(high)


def block_scale(own_key, shape, cuts, low, top_value):
    def one(dim, blocks):
        steps = jax.random.uniform(jax.random.fold_in(jax.random.fold_in(own_key, 6), dim), (blocks,), jnp.float32, low / len(cuts), top_value / len(cuts))
        return jnp.repeat(jnp.exp(steps), shape[dim] // blocks).reshape((-1,) + (1,) * (len(shape) - dim - 1))

    level = one(*cuts[0])
    for cut in cuts[1:]:
        level = level * one(*cut)
    return level


def scatter_about(rng, dims, spread, reach, pieces=(), kind=jnp.bfloat16):
    values = spread * jax.random.normal(rng, dims, jnp.float32)
    if pieces:
        values = values * block_scale(rng, dims, pieces, -0.22, 0.18)
    return jnp.clip(values, -reach, reach).astype(kind)


def setup_inputs(seed: int = 0) -> dict:
    key_of = jax.random.split(jax.random.key(seed), 10)
    features = scatter_about(key_of[0], (ROWS, F), 1.0, 6.0, ((0, 32),))
    embeddings = scatter_about(key_of[1], (ROWS, E), 1.0, 6.0, ((0, 32),))
    tile_values = scatter_about(key_of[2], (BLOCKS, K, TILE, TILE), 1.0, 4.0, ((0, 32),))
    tile_columns = plant(jax.random.randint(key_of[3], (BLOCKS, K), 0, ROWS_DEV // TILE + 2 * SEND_MOST), jax.random.fold_in(key_of[3], 1), 0, (ROWS_DEV // TILE + 2 * SEND_MOST) - 1).astype(jnp.int32)
    send_blocks = plant(jax.random.randint(key_of[4], (N_DOM, 2, SEND_MOST), 0, ROWS_DEV // TILE), jax.random.fold_in(key_of[4], 1), 0, (ROWS_DEV // TILE) - 1).astype(jnp.int32)
    send_count = draw_send_count(jax.random.fold_in(key_of[9], 71), 0)
    hub_rows = draw_hub_rows(jax.random.fold_in(key_of[9], 71), 0)
    hub_weight = scatter_about(key_of[7], (ROWS, HUBS), 1.0, 4.0, ((0, 32),))
    degree = plant(jax.random.randint(key_of[8], (ROWS,), 16, 65), jax.random.fold_in(key_of[8], 1), 16, 64).astype(jnp.int32)
    return {"features": features, "embeddings": embeddings, "tile_values": tile_values, "tile_columns": tile_columns, "send_blocks": send_blocks, "send_count": send_count, "hub_rows": hub_rows, "hub_weight": hub_weight, "degree": degree}


def reference(features, embeddings, tile_values, tile_columns, send_blocks, send_count, hub_rows, hub_weight, degree):
    feature_width = F + E
    block_count = ROWS_DEV // TILE
    device_count = N_DOM
    inverse_root = lax.rsqrt(degree.astype(jnp.float32)).reshape(device_count, ROWS_DEV, 1)
    current = jnp.concatenate([features, embeddings], axis=1).reshape(device_count, ROWS_DEV, feature_width)
    tiles_split = tile_values.reshape(device_count, block_count, K, TILE, TILE)
    columns_split = tile_columns.reshape(device_count, block_count, K).astype(jnp.int32)
    hubs_split = hub_rows.reshape(device_count, HUB_DEV).astype(jnp.int32)
    weight_split = hub_weight.reshape(device_count, ROWS_DEV, HUBS)
    live_slots = jnp.arange(SEND_MOST, dtype=jnp.int32)[None, None, :] < send_count[:, :, None]
    empty_rim = jnp.zeros((1, SEND_MOST, TILE, feature_width), jnp.bfloat16)
    results = []
    for hop_index in range(HOPS):
        scaled = (current.astype(jnp.float32) * inverse_root).astype(jnp.bfloat16)
        blocked = scaled.reshape(device_count, block_count, TILE, feature_width)
        outgoing = jax.vmap(lambda source, listed: source[listed])(blocked, send_blocks.astype(jnp.int32))
        outgoing = jnp.where(live_slots[:, :, :, None, None], outgoing, jnp.zeros_like(outgoing))
        from_left = jnp.concatenate([empty_rim, outgoing[:-1, 1]], axis=0)
        from_right = jnp.concatenate([outgoing[1:, 0], empty_rim], axis=0)
        extended = jnp.concatenate([blocked, from_left, from_right], axis=1)
        gathered_hubs = jax.vmap(lambda source, listed: source[listed])(scaled, hubs_split).reshape(HUBS, feature_width)

        def one_device(operands):
            buffer, tiles_here, columns_here, weight_here = operands
            picked = buffer[columns_here]
            local_part = jnp.einsum('bkij,bkjw->biw', tiles_here.astype(jnp.float32), picked.astype(jnp.float32))
            local_part = local_part.reshape(ROWS_DEV, feature_width)
            return local_part + jnp.dot(weight_here, gathered_hubs, preferred_element_type=jnp.float32)
        summed = lax.map(one_device, (extended, tiles_split, columns_split, weight_split))
        current = (summed * inverse_root).astype(jnp.bfloat16)
        results.append(current.reshape(ROWS, feature_width))
    stacked = jnp.stack(results)
    return (stacked[:, :, :F], stacked[:, :, F:])
```

```python
import functools

import jax
import jax.numpy as jnp
from jax import lax
from jax.experimental import pallas as pl
from jax.experimental.pallas import tpu as pltpu
from jax.sharding import PartitionSpec as P

HOPS = 3
VMEM = pltpu.VMEM
SMEM = pltpu.SMEM


def scale_rows(value, dmat):
    lanes = dmat.shape[1]
    pieces = [value[:, i : i + lanes] * dmat for i in range(0, value.shape[1], lanes)]
    return pieces[0] if len(pieces) == 1 else jnp.concatenate(pieces, axis=1)


def pack(parity, z_ref, blocks_ref, count_ref, hubs_ref, chip_ref, core_ref, hub_ref):
    send_most, tile, _ = chip_ref.shape
    for side, out_ref in ((parity, chip_ref), (1 - parity, core_ref)):
        for slot in range(send_most):
            block = z_ref[blocks_ref[0, side, slot]]
            live = slot < count_ref[0, side]
            out_ref[slot] = jnp.where(live, block, jnp.zeros_like(block))
    group = 16
    rows = []
    for i in range(hub_ref.shape[0]):
        row = hubs_ref[i]
        inside = row % tile
        base = pl.multiple_of(inside // group * group, group)
        near = z_ref[row // tile, pl.ds(base, group), :].astype(jnp.float32)
        at = lax.broadcasted_iota(jnp.int32, near.shape, 0) == inside % group
        rows.append(jnp.sum(jnp.where(at, near, 0.0), axis=0, keepdims=True))
    hub_ref[...] = jnp.concatenate(rows, axis=0).astype(jnp.bfloat16)


def prologue_kernel(
    index_ref, blocks_ref, count_ref, hubs_ref, degree_ref, features_ref, embeddings_ref,
    z_ref, dmat_ref, chip_ref, core_ref, hub_ref,
):
    blocks, tile, _ = z_ref.shape
    split = features_ref.shape[2]
    for b in range(blocks):
        root = lax.rsqrt(degree_ref[b : b + 1, :].astype(jnp.float32))
        dmat = jnp.broadcast_to(root, (tile, tile)).T
        dmat_ref[b] = dmat
        z_ref[b, :, :split] = scale_rows(features_ref[b].astype(jnp.float32), dmat).astype(jnp.bfloat16)
        z_ref[b, :, split:] = scale_rows(embeddings_ref[b].astype(jnp.float32), dmat).astype(jnp.bfloat16)
    pack(index_ref[0] % 2, z_ref, blocks_ref, count_ref, hubs_ref, chip_ref, core_ref, hub_ref)


def hop_kernel(
    index_ref, blocks_ref, count_ref, hubs_ref, columns_ref, tiles_ref, weight_ref, dmat_ref,
    z_ref, from_chip_ref, from_core_ref, gathered_ref, *refs, hop, last, write_at,
):
    refs = list(refs)
    if write_at:
        old_features, old_embeddings = refs[:2]
        refs = refs[2:]
        if write_at > 1:
            refs = refs[2:]
        all_features, all_embeddings = refs[:2]
        refs = refs[2:]
    if last:
        new_features, new_embeddings, extended, hub_sum, sems = refs
    else:
        new_features, new_embeddings, z_next, chip_ref, core_ref, hub_ref, extended, hub_sum, sems = refs
    copies = []
    if write_at:
        copies = [
            pltpu.make_async_copy(old_features, all_features.at[write_at - 1], sems.at[0]),
            pltpu.make_async_copy(old_embeddings, all_embeddings.at[write_at - 1], sems.at[1]),
        ]
        for copy in copies:
            copy.start()
    blocks, tile, width = z_ref.shape
    split = new_features.shape[2]
    per_block = columns_ref.shape[1]
    send_most = from_chip_ref.shape[0]
    parity = index_ref[0] % 2
    for b in range(blocks):
        extended[b] = z_ref[b]
    for slot in range(send_most):
        extended[blocks + parity * send_most + slot] = from_chip_ref[slot]
        extended[blocks + (1 - parity) * send_most + slot] = from_core_ref[slot]
    gathered = gathered_ref[...]
    for b in range(blocks):
        values = jnp.concatenate([tiles_ref[b, k] for k in range(per_block)], axis=1)
        picked = jnp.concatenate([extended[columns_ref[b, k]] for k in range(per_block)], axis=0)
        total = jnp.dot(values, picked, preferred_element_type=jnp.float32)
        total = total + jnp.dot(weight_ref[b], gathered, preferred_element_type=jnp.float32)
        dmat = dmat_ref[b]
        fresh = scale_rows(total, dmat).astype(jnp.bfloat16)
        new_features[b] = fresh[:, :split]
        new_embeddings[b] = fresh[:, split:]
        if last:
            row = 2 + 2 * b
            pair = [
                pltpu.make_async_copy(new_features.at[b], all_features.at[hop, b], sems.at[row]),
                pltpu.make_async_copy(new_embeddings.at[b], all_embeddings.at[hop, b], sems.at[row + 1]),
            ]
            for copy in pair:
                copy.start()
            copies += pair
        else:
            z_next[b] = scale_rows(fresh.astype(jnp.float32), dmat).astype(jnp.bfloat16)
    if not last:
        pack(parity, z_next, blocks_ref, count_ref, hubs_ref, chip_ref, core_ref, hub_ref)
    for copy in copies:
        copy.wait()


def body(
    features, embeddings, tile_values, tile_columns, send_blocks, send_count, hub_rows, hub_weight, degree,
):
    row_count, split = features.shape
    blocks, per_block, tile, _ = tile_values.shape
    extra = embeddings.shape[1]
    width = split + extra
    send_most = send_blocks.shape[2]
    hub_dev = hub_rows.shape[0]
    hub_total = hub_weight.shape[1]
    count = lax.axis_size("dom")
    bf16 = jnp.bfloat16

    index = lax.axis_index("dom").reshape(1)
    vmem = pl.BlockSpec(memory_space=VMEM)
    smem = pl.BlockSpec(memory_space=SMEM)
    hbm = pl.BlockSpec(memory_space=pl.ANY)
    params = pltpu.CompilerParams(vmem_limit_bytes=24 * 2**20)

    sends = [
        jax.ShapeDtypeStruct((send_most, tile, width), bf16),
        jax.ShapeDtypeStruct((send_most, tile, width), bf16),
        jax.ShapeDtypeStruct((hub_dev, width), bf16),
    ]
    z_shape = jax.ShapeDtypeStruct((blocks, tile, width), bf16)
    z, dmat, to_chip, to_core, hub = pl.pallas_call(
        prologue_kernel,
        out_shape=[z_shape, jax.ShapeDtypeStruct((blocks, tile, tile), jnp.float32)] + sends,
        in_specs=[smem] * 4 + [vmem] * 3,
        out_specs=[vmem] * 5,
        compiler_params=params,
        name="prologue",
    )(
        index, send_blocks, send_count, hub_rows,
        degree.reshape(blocks, tile),
        features.reshape(blocks, tile, split),
        embeddings.reshape(blocks, tile, extra),
    )

    core_pairs = [(i, i ^ 1) for i in range(count) if i ^ 1 < count]
    chip_pairs = [p for i in range(1, count - 1, 2) for p in ((i, i + 1), (i + 1, i))]
    weight = hub_weight.reshape(blocks, tile, hub_total)
    old = None
    out = None
    for hop in range(HOPS):
        last = hop == HOPS - 1
        from_chip = lax.ppermute(to_chip, "dom", chip_pairs)
        from_core = lax.ppermute(to_core, "dom", core_pairs)
        spread = jnp.broadcast_to(hub[None], (count, hub_dev, width))
        gathered = lax.all_to_all(spread, "dom", 0, 0).reshape(hub_total, width)
        operands = [index, send_blocks, send_count, hub_rows, tile_columns, tile_values, weight, dmat,
                    z, from_chip, from_core, gathered]
        in_specs = [smem] * 5 + [vmem] * 7
        fresh_shapes = [
            jax.ShapeDtypeStruct((blocks, tile, split), bf16),
            jax.ShapeDtypeStruct((blocks, tile, extra), bf16),
        ]
        whole_shapes = [
            jax.ShapeDtypeStruct((HOPS, blocks, tile, split), bf16),
            jax.ShapeDtypeStruct((HOPS, blocks, tile, extra), bf16),
        ]
        out_shape, out_specs, scratch, aliases = [], [], [], {}
        if hop:
            operands += list(old)
            in_specs += [vmem] * 2
            if hop > 1:
                aliases = {len(operands): 0, len(operands) + 1: 1}
                operands += list(out)
                in_specs += [hbm] * 2
            out_shape += whole_shapes
            out_specs += [hbm] * 2
        if last:
            scratch += [VMEM((blocks, tile, split), bf16), VMEM((blocks, tile, extra), bf16)]
        else:
            out_shape += fresh_shapes + [z_shape] + sends
            out_specs += [vmem] * 6
        scratch += [
            VMEM((blocks + 2 * send_most, tile, width), bf16),
            VMEM((8, 128), jnp.float32),
            pltpu.SemaphoreType.DMA((2 + 2 * blocks,)),
        ]
        got = pl.pallas_call(
            functools.partial(hop_kernel, hop=hop, last=last, write_at=hop),
            out_shape=out_shape,
            in_specs=in_specs,
            out_specs=out_specs,
            scratch_shapes=scratch,
            input_output_aliases=aliases,
            compiler_params=params,
            name=f"hop{hop}",
        )(*operands)
        if hop:
            out = got[:2]
            got = got[2:]
        if not last:
            old = got[:2]
            z, to_chip, to_core, hub = got[2:]
    return out[0].reshape(HOPS, row_count, split), out[1].reshape(HOPS, row_count, extra)


def solution(mesh):
    placed = (
        P("dom", None),
        P("dom", None),
        P("dom", None, None, None),
        P("dom", None),
        P("dom", None, None),
        P("dom", None),
        P("dom"),
        P("dom", None),
        P("dom"),
    )
    return jax.shard_map(
        body,
        mesh=mesh,
        in_specs=placed,
        out_specs=(P(None, "dom", None), P(None, "dom", None)),
        check_vma=False,
    )
```

```python
import functools

import jax
import jax.numpy as jnp
from jax import lax
from jax.experimental import pallas as pl
from jax.experimental.pallas import tpu as pltpu
from jax.sharding import PartitionSpec as P

HOPS = 3
VMEM = pltpu.VMEM
SMEM = pltpu.SMEM
BF16 = jnp.bfloat16
F32 = jnp.float32


def scale_rows(value, dmat):
    lanes = dmat.shape[1]
    pieces = [value[:, i : i + lanes] * dmat for i in range(0, value.shape[1], lanes)]
    return pieces[0] if len(pieces) == 1 else jnp.concatenate(pieces, axis=1)


def begin(copies):
    for copy in copies:
        copy.start()
    return copies


def finish(copies):
    for copy in copies:
        copy.wait()


def fetch(sources, targets, sems, first):
    return begin(
        [
            pltpu.make_async_copy(source, target, sems.at[first + i])
            for i, (source, target) in enumerate(zip(sources, targets))
        ]
    )


def pack(parity, z_ref, blocks_ref, count_ref, hubs_ref, chip_ref, core_ref, hub_ref):
    send_most, tile, _ = chip_ref.shape
    for side, out_ref in ((parity, chip_ref), (1 - parity, core_ref)):
        for slot in range(send_most):
            block = z_ref[blocks_ref[0, side, slot]]
            live = slot < count_ref[0, side]
            out_ref[slot] = jnp.where(live, block, jnp.zeros_like(block))
    group = 16
    rows = []
    for i in range(hub_ref.shape[0]):
        row = hubs_ref[i]
        inside = row % tile
        base = pl.multiple_of(inside // group * group, group)
        near = z_ref[row // tile, pl.ds(base, group), :].astype(F32)
        at = lax.broadcasted_iota(jnp.int32, near.shape, 0) == inside % group
        rows.append(jnp.sum(jnp.where(at, near, 0.0), axis=0, keepdims=True))
    hub_ref[...] = jnp.concatenate(rows, axis=0).astype(BF16)


def prologue_kernel(
    blocks_hbm, count_hbm, hubs_hbm, degree_hbm, features_hbm, embeddings_hbm,
    z_hbm, dmat_ref, chip_ref, core_ref, hub_ref,
    blocks_ref, count_ref, hubs_ref, degree_ref, features_ref, embeddings_ref, z_ref, sems,
):
    blocks, tile, _ = z_ref.shape
    split = features_ref.shape[2]
    writes = []
    degree_copy = fetch([degree_hbm], [degree_ref], sems, 0)
    row_copies = []
    for b in range(blocks):
        row_copies.append(
            fetch([features_hbm.at[b], embeddings_hbm.at[b]], [features_ref.at[b], embeddings_ref.at[b]],
                  sems, 4 + 2 * b)
        )
    tables = fetch([blocks_hbm, count_hbm, hubs_hbm], [blocks_ref, count_ref, hubs_ref], sems, 1)
    finish(degree_copy)
    for b in range(blocks):
        root = lax.rsqrt(degree_ref[b : b + 1, :].astype(F32))
        dmat = jnp.broadcast_to(root, (tile, tile)).T
        dmat_ref[b] = dmat
        finish(row_copies[b])
        z_ref[b, :, :split] = scale_rows(features_ref[b].astype(F32), dmat).astype(BF16)
        z_ref[b, :, split:] = scale_rows(embeddings_ref[b].astype(F32), dmat).astype(BF16)
        writes += fetch([z_ref.at[b]], [z_hbm.at[b]], sems, 4 + 2 * blocks + b)
    finish(tables)
    pack(lax.axis_index("dom") % 2, z_ref, blocks_ref, count_ref, hubs_ref, chip_ref, core_ref, hub_ref)
    finish(writes)


def own_kernel(columns_hbm, tiles_hbm, z_hbm, *refs, first):
    if first:
        weight_hbm, own_hbm, mixed_ref, columns_ref, tiles_ref, z_ref, weight_ref, own_ref, sems = refs
    else:
        own_hbm, columns_ref, tiles_ref, z_ref, own_ref, sems = refs
    blocks, tile, _ = z_ref.shape
    per_block = columns_ref.shape[0]
    table = fetch([columns_hbm], [columns_ref], sems, 0)
    rows = fetch([z_hbm], [z_ref], sems, 1)
    reads = [fetch([tiles_hbm.at[b]], [tiles_ref.at[b]], sems, 3 + b) for b in range(blocks)]
    if first:
        finish(fetch([weight_hbm], [weight_ref], sems, 2))
    finish(table)
    finish(rows)
    writes = []
    for b in range(blocks):
        finish(reads[b])
        columns = [columns_ref[k, b] for k in range(per_block)]
        tiles = [tiles_ref[b, k] for k in range(per_block)]
        values = jnp.concatenate(
            [jnp.where(c < blocks, t, jnp.zeros_like(t)) for c, t in zip(columns, tiles)], axis=1
        )
        picked = jnp.concatenate([z_ref[jnp.minimum(c, blocks - 1)] for c in columns], axis=0)
        own_ref[b] = jnp.dot(values, picked, preferred_element_type=F32)
        writes += fetch([own_ref.at[b]], [own_hbm.at[b]], sems, 3 + blocks + b)
        if first:
            rim = (mixed_ref.shape[2] - weight_ref.shape[0]) // tile
            for slot in range(rim):
                total = jnp.zeros((tile, tile), F32)
                for c, t in zip(columns, tiles):
                    total += jnp.where(c == blocks + slot, t, jnp.zeros_like(t)).astype(F32)
                mixed_ref[b, :, slot * tile : (slot + 1) * tile] = total.astype(BF16)
            mixed_ref[b, :, rim * tile :] = weight_ref[:, b * tile : (b + 1) * tile].astype(F32).T.astype(BF16)
    finish(writes)


def merge_kernel(
    blocks_hbm, count_hbm, hubs_hbm, own_hbm, mixed_ref, dmat_ref, from_chip_ref, from_core_ref, gathered_ref,
    *refs, hop, last,
):
    refs = list(refs)
    if hop:
        del refs[:2]
    all_features, all_embeddings = refs[:2]
    if last:
        new_features, new_embeddings, own_ref, received, sems = refs[2:]
    else:
        (z_hbm, chip_ref, core_ref, hub_ref, blocks_ref, count_ref, hubs_ref, z_next,
         new_features, new_embeddings, own_ref, received, sems) = refs[2:]
    blocks, tile, width = own_ref.shape
    reads = [fetch([own_hbm.at[b]], [own_ref.at[b]], sems, 3 + b) for b in range(blocks)]
    if not last:
        tables = fetch([blocks_hbm, count_hbm, hubs_hbm], [blocks_ref, count_ref, hubs_ref], sems, 0)
    split = new_features.shape[2]
    send_most = from_chip_ref.shape[0]
    rim_rows = send_most * tile
    parity = lax.axis_index("dom") % 2
    for slot in range(send_most):
        chip_at = pl.multiple_of(parity * rim_rows + slot * tile, tile)
        core_at = pl.multiple_of((1 - parity) * rim_rows + slot * tile, tile)
        received[pl.ds(chip_at, tile), :] = from_chip_ref[slot]
        received[pl.ds(core_at, tile), :] = from_core_ref[slot]
    received[2 * rim_rows :, :] = gathered_ref[...]
    writes = []
    for b in range(blocks):
        total = jnp.dot(mixed_ref[b], received[...], preferred_element_type=F32)
        finish(reads[b])
        total = own_ref[b] + total
        dmat = dmat_ref[b]
        fresh = scale_rows(total, dmat).astype(BF16)
        new_features[b] = fresh[:, :split]
        new_embeddings[b] = fresh[:, split:]
        sources = [new_features.at[b], new_embeddings.at[b]]
        targets = [all_features.at[hop, b], all_embeddings.at[hop, b]]
        if not last:
            z_next[b] = scale_rows(fresh.astype(F32), dmat).astype(BF16)
            sources.append(z_next.at[b])
            targets.append(z_hbm.at[b])
        writes += fetch(sources, targets, sems, 3 + blocks + 3 * b)
    if not last:
        finish(tables)
        pack(parity, z_next, blocks_ref, count_ref, hubs_ref, chip_ref, core_ref, hub_ref)
    finish(writes)


def body(
    features, embeddings, tile_values, tile_columns, send_blocks, send_count, hub_rows, hub_weight, degree,
):
    row_count, split = features.shape
    blocks, per_block, tile, _ = tile_values.shape
    extra = embeddings.shape[1]
    width = split + extra
    send_most = send_blocks.shape[2]
    hub_dev = hub_rows.shape[0]
    hub_total = hub_weight.shape[1]
    count = lax.axis_size("dom")
    rim_rows = 2 * send_most * tile

    vmem = pl.BlockSpec(memory_space=VMEM)
    hbm = pl.BlockSpec(memory_space=pltpu.HBM)
    shape = jax.ShapeDtypeStruct

    def pin(*values):
        return [pltpu.with_memory_space_constraint(value, pltpu.HBM) for value in values]

    def call(kernel, name, flops, **kwargs):
        return pl.pallas_call(
            kernel,
            name=name,
            compiler_params=pltpu.CompilerParams(vmem_limit_bytes=24 * 2**20),
            cost_estimate=pl.CostEstimate(flops=flops, bytes_accessed=0, transcendentals=0),
            **kwargs,
        )

    int32 = jnp.int32
    tables = [SMEM(send_blocks.shape, int32), SMEM(send_count.shape, int32), SMEM(hub_rows.shape, int32)]
    sends = [
        shape((send_most, tile, width), BF16), shape((send_most, tile, width), BF16), shape((hub_dev, width), BF16),
    ]
    whole = [pltpu.HBM((HOPS, blocks, tile, split), BF16), pltpu.HBM((HOPS, blocks, tile, extra), BF16)]
    z_like = (blocks, tile, width)
    lists = pin(send_blocks, send_count, hub_rows)
    z, dmat, to_chip, to_core, hub = call(
        prologue_kernel, "prologue", 10**8,
        out_shape=[pltpu.HBM(z_like, BF16), shape((blocks, tile, tile), F32)] + sends,
        in_specs=[hbm] * 6,
        out_specs=[hbm] + [vmem] * 4,
        scratch_shapes=tables + [
            VMEM((blocks, tile), int32), VMEM((blocks, tile, split), BF16), VMEM((blocks, tile, extra), BF16),
            VMEM(z_like, BF16), pltpu.SemaphoreType.DMA((4 + 3 * blocks,)),
        ],
    )(
        *lists,
        *pin(degree.reshape(blocks, tile), features.reshape(blocks, tile, split),
             embeddings.reshape(blocks, tile, extra)),
    )

    core_pairs = [(i, i ^ 1) for i in range(count) if i ^ 1 < count]
    chip_pairs = [p for i in range(1, count - 1, 2) for p in ((i, i + 1), (i + 1, i))]
    fixed = pin(tile_columns.T, tile_values)
    mixed = out = None
    for hop in range(HOPS):
        first, last = hop == 0, hop == HOPS - 1
        from_chip = lax.ppermute(to_chip, "dom", chip_pairs)
        from_core = lax.ppermute(to_core, "dom", core_pairs)
        spread = jnp.broadcast_to(hub[None], (count, hub_dev, width))
        gathered = lax.all_to_all(spread, "dom", 0, 0).reshape(hub_total, width)

        operands = fixed + pin(z)
        out_shape, out_specs = [pltpu.HBM(z_like, F32)], [hbm]
        scratch = [
            SMEM((per_block, blocks), int32), VMEM(tile_values.shape, BF16), VMEM(z_like, BF16),
            VMEM(z_like, F32), pltpu.SemaphoreType.DMA((3 + 2 * blocks,)),
        ]
        if first:
            operands += pin(hub_weight.T)
            out_shape += [shape((blocks, tile, rim_rows + hub_total), BF16)]
            out_specs += [vmem]
            scratch.insert(3, VMEM((hub_total, row_count), BF16))
        own, *rest = call(
            functools.partial(own_kernel, first=first), f"own{hop}", 2 * row_count * per_block * tile * width,
            out_shape=out_shape, in_specs=[hbm] * len(operands), out_specs=out_specs, scratch_shapes=scratch,
        )(*operands)
        if first:
            (mixed,) = rest

        operands = lists + pin(own) + [mixed, dmat, from_chip, from_core, gathered]
        in_specs = [hbm] * 4 + [vmem] * 5
        aliases = {}
        if hop:
            aliases = {len(operands): 0, len(operands) + 1: 1}
            operands += pin(*out)
            in_specs += [hbm] * 2
        out_shape, out_specs = list(whole), [hbm] * 2
        scratch = [
            VMEM((blocks, tile, split), BF16), VMEM((blocks, tile, extra), BF16), VMEM(z_like, F32),
            VMEM((rim_rows + hub_total, width), BF16), pltpu.SemaphoreType.DMA((3 + 4 * blocks,)),
        ]
        if not last:
            out_shape += [pltpu.HBM(z_like, BF16)] + sends
            out_specs += [hbm] + [vmem] * 3
            scratch = tables + [VMEM(z_like, BF16)] + scratch
        got = call(
            functools.partial(merge_kernel, hop=hop, last=last), f"merge{hop}",
            2 * row_count * (rim_rows + hub_total) * width,
            out_shape=out_shape, in_specs=in_specs, out_specs=out_specs, input_output_aliases=aliases,
            scratch_shapes=scratch,
        )(*operands)
        out = got[:2]
        if not last:
            z, to_chip, to_core, hub = got[2:]
    return out[0].reshape(HOPS, row_count, split), out[1].reshape(HOPS, row_count, extra)


def solution(mesh):
    placed = (
        P("dom", None),
        P("dom", None),
        P("dom", None, None, None),
        P("dom", None),
        P("dom", None, None),
        P("dom", None),
        P("dom"),
        P("dom", None),
        P("dom"),
    )
    return jax.shard_map(
        body,
        mesh=mesh,
        in_specs=placed,
        out_specs=(P(None, "dom", None), P(None, "dom", None)),
        check_vma=False,
    )
```

```python
import functools

import jax
import jax.numpy as jnp
from jax import lax
from jax.experimental import pallas as pl
from jax.experimental.pallas import tpu as pltpu
from jax.sharding import PartitionSpec as P

HOPS = 3
VMEM = pltpu.VMEM
SMEM = pltpu.SMEM
BF16 = jnp.bfloat16
F32 = jnp.float32
GROUP = 16


def scale_rows(value, dmat):
    lanes = dmat.shape[1]
    pieces = [value[:, i : i + lanes] * dmat for i in range(0, value.shape[1], lanes)]
    return pieces[0] if len(pieces) == 1 else jnp.concatenate(pieces, axis=1)


def finish(copies):
    for copy in copies:
        copy.wait()


class Copies:
    def __init__(self, sems):
        self.sems, self.used = sems, 0

    def start(self, *pairs):
        begun = []
        for source, target in pairs:
            copy = pltpu.make_async_copy(source, target, self.sems.at[self.used])
            copy.start()
            begun.append(copy)
            self.used += 1
        return begun


def block_rows(index, tile):
    return pl.ds(pl.multiple_of(index * tile, tile), tile)


def one_row(ref, row):
    base = pl.multiple_of(row // GROUP * GROUP, GROUP)
    near = ref[pl.ds(base, GROUP), :].astype(F32)
    at = lax.broadcasted_iota(jnp.int32, near.shape, 0) == row % GROUP
    return jnp.sum(jnp.where(at, near, 0.0), axis=0, keepdims=True)


def factor_block(degree_ref, index):
    tile = degree_ref.shape[1]
    root = lax.rsqrt(degree_ref[pl.ds(index, 1), :].astype(F32))
    return jnp.broadcast_to(root, (tile, tile)).T


def slots(blocks_ref, count_ref):
    parity = lax.axis_index("dom") % 2
    send_most = blocks_ref.shape[2]
    return [
        (blocks_ref[0, side, slot], slot < count_ref[0, side])
        for side in (parity, 1 - parity)
        for slot in range(send_most)
    ]


def gather_sent(source_ref, target_ref, listed, hubs_ref):
    tile = (target_ref.shape[0] - GROUP) // len(listed)
    width = source_ref.shape[1]
    for i, (index, live) in enumerate(listed):
        block = source_ref[block_rows(index, tile), :]
        target_ref[i * tile : (i + 1) * tile, :] = jnp.where(live, block, jnp.zeros_like(block))
    rows = [one_row(source_ref, hubs_ref[i]) for i in range(hubs_ref.shape[0])]
    rows.append(jnp.zeros((GROUP - len(rows), width), F32))
    target_ref[len(listed) * tile :, :] = jnp.concatenate(rows, axis=0).astype(target_ref.dtype)


def place_received(from_chip_ref, from_core_ref, gathered_ref, received):
    rim_rows = from_chip_ref.shape[0]
    parity = lax.axis_index("dom") % 2
    received[block_rows(parity, rim_rows), :] = from_chip_ref[...]
    received[block_rows(1 - parity, rim_rows), :] = from_core_ref[...]
    received[2 * rim_rows :, :] = gathered_ref[...]


def prologue_kernel(
    blocks_hbm, count_hbm, hubs_hbm, degree_hbm, features_hbm, embeddings_hbm,
    chip_ref, core_ref, spread_ref,
    blocks_ref, count_ref, hubs_ref, degree_ref, features_ref, embeddings_ref, sems,
):
    copies = Copies(sems)
    tile = degree_ref.shape[1]
    split = features_ref.shape[1]
    tables = copies.start(
        (blocks_hbm, blocks_ref), (count_hbm, count_ref), (hubs_hbm, hubs_ref), (degree_hbm, degree_ref)
    )
    rows = copies.start((features_hbm, features_ref), (embeddings_hbm, embeddings_ref))
    finish(tables)
    listed = slots(blocks_ref, count_ref)
    factors = [factor_block(degree_ref, index) for index, _ in listed]
    finish(rows)
    half = len(listed) // 2
    for i, (index, live) in enumerate(listed):
        target = (chip_ref, core_ref)[i // half]
        into = slice((i % half) * tile, (i % half + 1) * tile)
        for source, columns in ((features_ref, slice(0, split)), (embeddings_ref, slice(split, None))):
            block = scale_rows(source[block_rows(index, tile), :].astype(F32), factors[i])
            target[into, columns] = jnp.where(live, block, 0.0).astype(BF16)
    rows = []
    for i in range(hubs_ref.shape[0]):
        row = hubs_ref[i]
        degrees = degree_ref[pl.ds(row // tile, 1), :].astype(F32)
        at = lax.broadcasted_iota(jnp.int32, degrees.shape, 1) == row % tile
        factor = lax.rsqrt(jnp.broadcast_to(jnp.sum(jnp.where(at, degrees, 0.0), axis=1, keepdims=True), (1, tile)))
        whole = jnp.concatenate([one_row(features_ref, row), one_row(embeddings_ref, row)], axis=1)
        rows.append(scale_rows(whole, factor))
    hub = jnp.concatenate(rows, axis=0).astype(BF16)
    spread_ref[...] = jnp.broadcast_to(hub[None], spread_ref.shape)


def bulk_kernel(*refs, hop, rim, per_block):
    refs = list(refs)
    take = lambda n: [refs.pop(0) for _ in range(n)]
    blocks_hbm, count_hbm, hubs_hbm, columns_hbm, tiles_hbm = take(5)
    first, last = hop == 0, hop == HOPS - 1
    if first:
        degree_hbm, features_hbm, embeddings_hbm, weight_hbm = take(4)
        own_hbm, own_sent_hbm, mixed_out, dmat_out, mixed_sent, dmat_sent = take(6)
    else:
        old_own_hbm, mixed_hbm, dmat_hbm, received_hbm = take(4)
        if hop > 1:
            take(2)
        all_features, all_embeddings, own_hbm = take(3)
        if last:
            mixed_out, dmat_out = take(2)
        else:
            (own_sent_hbm,) = take(1)
    blocks_ref, count_ref, hubs_ref, columns_ref = take(4)
    tiles_ref, z_ref, own_ref, own_sent, mixed_ref, dmat_ref, features_ref, embeddings_ref = take(8)
    if first:
        degree_ref, weight_ref, sems = refs
    else:
        received, sems = refs
    copies = Copies(sems)
    blocks, _, tile, _ = tiles_ref.shape
    row_count, width = z_ref.shape
    split = features_ref.shape[1]
    half = row_count // 2
    halves = (slice(0, half), slice(half, row_count))

    tables = copies.start(
        (blocks_hbm, blocks_ref), (count_hbm, count_ref), (hubs_hbm, hubs_ref), (columns_hbm, columns_ref)
    )
    writes = []
    if first:
        inputs = copies.start((degree_hbm, degree_ref), (features_hbm, features_ref),
                              (embeddings_hbm, embeddings_ref))
        late = copies.start((tiles_hbm, tiles_ref), (weight_hbm, weight_ref))
        finish(inputs)
    else:
        inputs = copies.start((received_hbm, received), (mixed_hbm, mixed_ref), (dmat_hbm, dmat_ref))
        olds = [copies.start((old_own_hbm.at[h, :], own_ref.at[h, :])) for h in halves]
        late = copies.start((tiles_hbm, tiles_ref))
        finish(inputs)
    for b in range(blocks):
        rows = slice(b * tile, (b + 1) * tile)
        if first:
            dmat = factor_block(degree_ref, b)
            dmat_ref[rows, :] = dmat
            z_ref[rows, :split] = scale_rows(features_ref[rows, :].astype(F32), dmat).astype(BF16)
            z_ref[rows, split:] = scale_rows(embeddings_ref[rows, :].astype(F32), dmat).astype(BF16)
        else:
            total = jnp.dot(mixed_ref[rows, :], received[...], preferred_element_type=F32)
            if b * tile in (0, half):
                finish(olds[b * tile // half])
            dmat = dmat_ref[rows, :]
            fresh = scale_rows(own_ref[rows, :] + total, dmat).astype(BF16)
            features_ref[rows, :] = fresh[:, :split]
            embeddings_ref[rows, :] = fresh[:, split:]
            z_ref[rows, :] = scale_rows(fresh.astype(F32), dmat).astype(BF16)
    if not first:
        writes += copies.start(
            (features_ref, all_features.at[hop - 1]), (embeddings_ref, all_embeddings.at[hop - 1])
        )
    finish(late)
    finish(tables)
    for b in range(blocks):
        rows = slice(b * tile, (b + 1) * tile)
        columns = [columns_ref[k, b] for k in range(per_block)]
        tiles = [tiles_ref[b, k] for k in range(per_block)]
        values = jnp.concatenate(
            [jnp.where(c < blocks, t, jnp.zeros_like(t)) for c, t in zip(columns, tiles)], axis=1
        )
        picked = jnp.concatenate([z_ref[block_rows(jnp.minimum(c, blocks - 1), tile), :] for c in columns], axis=0)
        own_ref[rows, :] = jnp.dot(values, picked, preferred_element_type=F32)
        writes += copies.start((own_ref.at[rows, :], own_hbm.at[rows, :]))
        if first:
            for slot in range(rim):
                total = jnp.zeros((tile, tile), F32)
                for c, t in zip(columns, tiles):
                    total += jnp.where(c == blocks + slot, t, jnp.zeros_like(t)).astype(F32)
                mixed_ref[rows, slot * tile : (slot + 1) * tile] = total.astype(BF16)
            mixed_ref[rows, rim * tile :] = weight_ref[:, rows].astype(F32).T.astype(BF16)
    if not last:
        listed = slots(blocks_ref, count_ref)
        gather_sent(own_ref, own_sent, listed, hubs_ref)
        writes += copies.start((own_sent, own_sent_hbm))
    if first:
        writes += copies.start((mixed_ref, mixed_out), (dmat_ref, dmat_out))
        gather_sent(mixed_ref, mixed_sent, listed, hubs_ref)
        gather_sent(dmat_ref, dmat_sent, listed, hubs_ref)
    if last:
        mixed_out[...] = mixed_ref[...]
        dmat_out[...] = dmat_ref[...]
    finish(writes)


def edge_kernel(
    own_hbm, mixed_ref, dmat_ref, from_chip_ref, from_core_ref, gathered_ref,
    chip_ref, core_ref, spread_ref, received_hbm,
    own_ref, received, sems,
):
    copies = Copies(sems)
    rim_rows = chip_ref.shape[0]
    hub_dev = spread_ref.shape[1]
    parts = [slice(0, rim_rows), slice(rim_rows, own_ref.shape[0])]
    reads = [copies.start((own_hbm.at[part, :], own_ref.at[part, :])) for part in parts]
    place_received(from_chip_ref, from_core_ref, gathered_ref, received)
    writes = copies.start((received, received_hbm))
    for part, read in zip(parts, reads):
        total = jnp.dot(mixed_ref[part, :], received[...], preferred_element_type=F32)
        finish(read)
        dmat = dmat_ref[part, :]
        fresh = scale_rows(own_ref[part, :] + total, dmat).astype(BF16)
        sent = scale_rows(fresh.astype(F32), dmat)
        if part.start == 0:
            chip_ref[...] = sent.astype(BF16)
        else:
            core_ref[...] = sent[:rim_rows].astype(BF16)
            hub = sent[rim_rows : rim_rows + hub_dev].astype(BF16)
            spread_ref[...] = jnp.broadcast_to(hub[None], spread_ref.shape)
    finish(writes)


def final_kernel(
    own_hbm, mixed_ref, dmat_ref, from_chip_ref, from_core_ref, gathered_ref, _, __,
    all_features, all_embeddings,
    own_ref, features_ref, embeddings_ref, received, sems,
):
    copies = Copies(sems)
    tile = dmat_ref.shape[1]
    split = features_ref.shape[1]
    blocks = [slice(i, i + tile) for i in range(0, own_ref.shape[0], tile)]
    reads = [copies.start((own_hbm.at[rows, :], own_ref.at[rows, :])) for rows in blocks]
    place_received(from_chip_ref, from_core_ref, gathered_ref, received)
    writes = []
    for rows, read in zip(blocks, reads):
        total = jnp.dot(mixed_ref[rows, :], received[...], preferred_element_type=F32)
        finish(read)
        fresh = scale_rows(own_ref[rows, :] + total, dmat_ref[rows, :]).astype(BF16)
        features_ref[rows, :] = fresh[:, :split]
        embeddings_ref[rows, :] = fresh[:, split:]
        writes += copies.start(
            (features_ref.at[rows, :], all_features.at[HOPS - 1, rows, :]),
            (embeddings_ref.at[rows, :], all_embeddings.at[HOPS - 1, rows, :]),
        )
    finish(writes)


def body(
    features, embeddings, tile_values, tile_columns, send_blocks, send_count, hub_rows, hub_weight, degree,
):
    row_count, split = features.shape
    blocks, per_block, tile, _ = tile_values.shape
    extra = embeddings.shape[1]
    width = split + extra
    send_most = send_blocks.shape[2]
    hub_dev = hub_rows.shape[0]
    hub_total = hub_weight.shape[1]
    count = lax.axis_size("dom")
    rim = 2 * send_most
    deep = rim * tile + hub_total
    sent = rim * tile + GROUP

    vmem = pl.BlockSpec(memory_space=VMEM)
    hbm = pl.BlockSpec(memory_space=pltpu.HBM)
    shape = jax.ShapeDtypeStruct
    int32 = jnp.int32

    def pin(*values):
        return [pltpu.with_memory_space_constraint(value, pltpu.HBM) for value in values]

    def call(kernel, name, flops, out_shape, scratch, sems, in_hbm, operands, aliases={}):
        specs = [hbm] * in_hbm + [vmem] * (len(operands) - in_hbm)
        for source in aliases:
            specs[source] = hbm
        return pl.pallas_call(
            kernel,
            name=name,
            out_shape=out_shape,
            in_specs=specs,
            out_specs=[vmem if isinstance(out, shape) else hbm for out in out_shape],
            scratch_shapes=scratch + [pltpu.SemaphoreType.DMA((sems,))],
            input_output_aliases=aliases,
            compiler_params=pltpu.CompilerParams(vmem_limit_bytes=32 * 2**20),
            cost_estimate=pl.CostEstimate(flops=flops, bytes_accessed=0, transcendentals=0),
        )(*operands)

    tables = [SMEM(send_blocks.shape, int32), SMEM(send_count.shape, int32), SMEM(hub_rows.shape, int32)]
    sends = [
        shape((send_most * tile, width), BF16), shape((send_most * tile, width), BF16),
        shape((count, hub_dev, width), BF16),
    ]
    whole = [pltpu.HBM((HOPS, row_count, split), BF16), pltpu.HBM((HOPS, row_count, extra), BF16)]
    row_buffers = [VMEM((row_count, split), BF16), VMEM((row_count, extra), BF16)]
    lists = pin(send_blocks, send_count, hub_rows)
    rows = pin(degree.reshape(blocks, tile), features, embeddings)
    to_chip, to_core, spread = call(
        prologue_kernel, "prologue", 10**8, sends,
        tables + [VMEM((blocks, tile), int32)] + row_buffers, 6, 6, lists + rows,
    )

    core_pairs = [(i, i ^ 1) for i in range(count) if i ^ 1 < count]
    chip_pairs = [p for i in range(1, count - 1, 2) for p in ((i, i + 1), (i + 1, i))]
    fixed = lists + pin(tile_columns.T, tile_values)
    out = []
    for hop in range(HOPS):
        first, last = hop == 0, hop == HOPS - 1
        from_chip = lax.ppermute(to_chip, "dom", chip_pairs)
        from_core = lax.ppermute(to_core, "dom", core_pairs)
        gathered = lax.all_to_all(spread, "dom", 0, 0).reshape(hub_total, width)

        scratch = tables + [
            SMEM((per_block, blocks), int32), VMEM(tile_values.shape, BF16), VMEM((row_count, width), BF16),
            VMEM((row_count, width), F32), VMEM((sent, width), F32),
            VMEM((row_count, deep), BF16), VMEM((row_count, tile), F32),
        ] + row_buffers
        aliases = {}
        full_own = pltpu.HBM((row_count, width), F32)
        sent_own = pltpu.HBM((sent, width), F32)
        if first:
            operands = fixed + rows + pin(hub_weight.T)
            out_shape = [full_own, sent_own, pltpu.HBM((row_count, deep), BF16), pltpu.HBM((row_count, tile), F32),
                         shape((sent, deep), BF16), shape((sent, tile), F32)]
            scratch += [VMEM((blocks, tile), int32), VMEM((hub_total, row_count), BF16)]
        else:
            operands = fixed + pin(own, mixed, dmat, received)
            if out:
                aliases = {len(operands): 0, len(operands) + 1: 1}
                operands += pin(*out)
            out_shape = whole + [full_own]
            out_shape += [shape((row_count, deep), BF16), shape((row_count, tile), F32)] if last else [sent_own]
            scratch += [VMEM((deep, width), BF16)]
        got = call(
            functools.partial(bulk_kernel, hop=hop, rim=rim, per_block=per_block), f"bulk{hop}",
            4 * row_count * per_block * tile * width, out_shape, scratch, 16 + blocks,
            len(operands), operands, aliases,
        )
        if first:
            own, own_sent, mixed, dmat, mixed_sent, dmat_sent = got
        else:
            out, (own, *got) = got[:2], got[2:]
            if last:
                mixed_here, dmat_here = got
            else:
                (own_sent,) = got

        flops = 2 * row_count * deep * width
        if last:
            operands = pin(own) + [mixed_here, dmat_here, from_chip, from_core, gathered]
            aliases = {len(operands): 0, len(operands) + 1: 1}
            out = call(
                final_kernel, "final", flops, whole,
                [VMEM((row_count, width), F32)] + row_buffers + [VMEM((deep, width), BF16)], 3 * blocks,
                1, operands + pin(*out), aliases,
            )
        else:
            to_chip, to_core, spread, received = call(
                edge_kernel, f"edge{hop}", flops, sends + [pltpu.HBM((deep, width), BF16)],
                [VMEM((sent, width), F32), VMEM((deep, width), BF16)], 3,
                1, pin(own_sent) + [mixed_sent, dmat_sent, from_chip, from_core, gathered],
            )
    return out[0], out[1]


def solution(mesh):
    placed = (
        P("dom", None),
        P("dom", None),
        P("dom", None, None, None),
        P("dom", None),
        P("dom", None, None),
        P("dom", None),
        P("dom"),
        P("dom", None),
        P("dom"),
    )
    return jax.shard_map(
        body,
        mesh=mesh,
        in_specs=placed,
        out_specs=(P(None, "dom", None), P(None, "dom", None)),
        check_vma=False,
    )
```

```python
import functools

import jax
import jax.numpy as jnp
from jax import lax
from jax.experimental import pallas as pl
from jax.experimental.pallas import tpu as pltpu
from jax.sharding import PartitionSpec as P

HOPS = 3
VMEM = pltpu.VMEM
SMEM = pltpu.SMEM
BF16 = jnp.bfloat16
F32 = jnp.float32
GROUP = 16


def scale_rows(value, dmat):
    lanes = dmat.shape[1]
    pieces = [value[:, i : i + lanes] * dmat for i in range(0, value.shape[1], lanes)]
    return pieces[0] if len(pieces) == 1 else jnp.concatenate(pieces, axis=1)


def finish(copies):
    for copy in copies:
        copy.wait()


class Copies:
    def __init__(self, sems):
        self.sems, self.used = sems, 0

    def start(self, *pairs):
        begun = []
        for source, target in pairs:
            copy = pltpu.make_async_copy(source, target, self.sems.at[self.used])
            copy.start()
            begun.append(copy)
            self.used += 1
        return begun


def block_rows(index, tile):
    return pl.ds(pl.multiple_of(index * tile, tile), tile)


def one_row(ref, row):
    base = pl.multiple_of(row // GROUP * GROUP, GROUP)
    near = ref[pl.ds(base, GROUP), :].astype(F32)
    at = lax.broadcasted_iota(jnp.int32, near.shape, 0) == row % GROUP
    return jnp.sum(jnp.where(at, near, 0.0), axis=0, keepdims=True)


def lane_to_rows(root):
    return jnp.broadcast_to(root, (root.shape[1], root.shape[1])).T


def roots_of(degree_ref, index):
    return lax.rsqrt(degree_ref[pl.ds(index, 1), :].astype(F32))


def factor_block(degree_ref, index):
    return lane_to_rows(roots_of(degree_ref, index))


def hub_roots(degree_ref, hubs_ref):
    tile = degree_ref.shape[1]
    found = []
    for i in range(hubs_ref.shape[0]):
        roots = roots_of(degree_ref, hubs_ref[i] // tile)
        at = lax.broadcasted_iota(jnp.int32, roots.shape, 1) == hubs_ref[i] % tile
        found.append(jnp.sum(jnp.where(at, roots, 0.0), axis=1, keepdims=True))
    return found


def gather_roots(degree_ref, roots_ref, listed, hubs_ref):
    tile = degree_ref.shape[1]
    rows = [roots_of(degree_ref, index) for index, _ in listed]
    lane = lax.broadcasted_iota(jnp.int32, (1, tile), 1)
    last = jnp.zeros((1, tile), F32)
    for i, root in enumerate(hub_roots(degree_ref, hubs_ref)):
        last = jnp.where(lane == i, jnp.broadcast_to(root, (1, tile)), last)
    roots_ref[...] = jnp.concatenate(rows + [last], axis=0)


def quarters(row_count):
    part = row_count // 4
    return [slice(i, i + part) for i in range(0, row_count, part)]


def slots(blocks_ref, count_ref):
    parity = lax.axis_index("dom") % 2
    send_most = blocks_ref.shape[2]
    return [
        (blocks_ref[0, side, slot], slot < count_ref[0, side])
        for side in (parity, 1 - parity)
        for slot in range(send_most)
    ]


def gather_sent(source_ref, target_ref, listed, hubs_ref):
    tile = (target_ref.shape[0] - GROUP) // len(listed)
    width = source_ref.shape[1]
    for i, (index, live) in enumerate(listed):
        block = source_ref[block_rows(index, tile), :]
        target_ref[i * tile : (i + 1) * tile, :] = jnp.where(live, block, jnp.zeros_like(block))
    rows = [one_row(source_ref, hubs_ref[i]) for i in range(hubs_ref.shape[0])]
    rows.append(jnp.zeros((GROUP - len(rows), width), F32))
    target_ref[len(listed) * tile :, :] = jnp.concatenate(rows, axis=0).astype(target_ref.dtype)


def place_received(from_chip_ref, from_core_ref, gathered_ref, received):
    rim_rows = from_chip_ref.shape[0]
    parity = lax.axis_index("dom") % 2
    received[block_rows(parity, rim_rows), :] = from_chip_ref[...]
    received[block_rows(1 - parity, rim_rows), :] = from_core_ref[...]
    received[2 * rim_rows :, :] = gathered_ref[...]


def spread_rows(rows, spread_ref, spread_hbm, copies):
    spread_ref[...] = jnp.broadcast_to(rows[None], spread_ref.shape)
    return copies.start((spread_ref, spread_hbm))


def prologue_kernel(
    blocks_hbm, count_hbm, hubs_hbm, degree_hbm, features_hbm, embeddings_hbm,
    chip_ref, core_ref, spread_hbm,
    blocks_ref, count_ref, hubs_ref, degree_ref, features_ref, embeddings_ref, spread_ref, sems,
):
    copies = Copies(sems)
    tile = degree_ref.shape[1]
    split = features_ref.shape[1]
    tables = copies.start(
        (blocks_hbm, blocks_ref), (count_hbm, count_ref), (hubs_hbm, hubs_ref), (degree_hbm, degree_ref)
    )
    rows = copies.start((features_hbm, features_ref), (embeddings_hbm, embeddings_ref))
    finish(tables)
    listed = slots(blocks_ref, count_ref)
    factors = [factor_block(degree_ref, index) for index, _ in listed]
    finish(rows)
    hubs = []
    for i, root in enumerate(hub_roots(degree_ref, hubs_ref)):
        row = hubs_ref[i]
        whole = jnp.concatenate([one_row(features_ref, row), one_row(embeddings_ref, row)], axis=1)
        hubs.append(scale_rows(whole, jnp.broadcast_to(root, (1, tile))))
    writes = spread_rows(jnp.concatenate(hubs, axis=0).astype(BF16), spread_ref, spread_hbm, copies)
    half = len(listed) // 2
    for i, (index, live) in enumerate(listed):
        target = (chip_ref, core_ref)[i // half]
        into = slice((i % half) * tile, (i % half + 1) * tile)
        for source, columns in ((features_ref, slice(0, split)), (embeddings_ref, slice(split, None))):
            block = scale_rows(source[block_rows(index, tile), :].astype(F32), factors[i])
            target[into, columns] = jnp.where(live, block, 0.0).astype(BF16)
    finish(writes)


def bulk_kernel(*refs, hop, rim, per_block):
    refs = list(refs)
    take = lambda n: [refs.pop(0) for _ in range(n)]
    blocks_hbm, count_hbm, hubs_hbm, columns_hbm, tiles_hbm = take(5)
    first, last = hop == 0, hop == HOPS - 1
    if first:
        degree_hbm, features_hbm, embeddings_hbm, weight_hbm = take(4)
        own_hbm, own_sent, mixed_out, dmat_out, mixed_sent, roots_sent = take(6)
    else:
        old_own_hbm, mixed_hbm, dmat_hbm, received_hbm = take(4)
        if hop > 1:
            take(2)
        all_features, all_embeddings, own_hbm = take(3)
        if last:
            mixed_ref, dmat_ref = take(2)
        else:
            (own_sent,) = take(1)
    blocks_ref, count_ref, hubs_ref, columns_ref = take(4)
    tiles_ref, z_ref, own_ref, features_ref, embeddings_ref = take(5)
    if not last:
        mixed_ref, dmat_ref = take(2)
    if first:
        degree_ref, weight_ref, sems = refs
    else:
        received, old_own_ref, total_ref, sems = refs
    copies = Copies(sems)
    blocks, _, tile, _ = tiles_ref.shape
    row_count, width = z_ref.shape
    split = features_ref.shape[1]
    every = [slice(b * tile, (b + 1) * tile) for b in range(blocks)]

    tables = copies.start((columns_hbm, columns_ref))
    if not last:
        tables += copies.start((blocks_hbm, blocks_ref), (count_hbm, count_ref), (hubs_hbm, hubs_ref))
    writes = []
    if first:
        finish(copies.start((degree_hbm, degree_ref), (features_hbm, features_ref),
                            (embeddings_hbm, embeddings_ref)))
        late = copies.start((tiles_hbm, tiles_ref), (weight_hbm, weight_ref))
        for b, rows in enumerate(every):
            dmat = factor_block(degree_ref, b)
            dmat_ref[rows, :] = dmat
            z_ref[rows, :split] = scale_rows(features_ref[rows, :].astype(F32), dmat).astype(BF16)
            z_ref[rows, split:] = scale_rows(embeddings_ref[rows, :].astype(F32), dmat).astype(BF16)
    else:
        parts = quarters(row_count)
        finish_first = copies.start((received_hbm, received))
        mixes = [copies.start((mixed_hbm.at[rows, :], mixed_ref.at[rows, :])) for rows in parts]
        rest = copies.start((dmat_hbm, dmat_ref), (old_own_hbm, old_own_ref))
        late = copies.start((tiles_hbm, tiles_ref))
        finish(finish_first)
        for rows, mix in zip(parts, mixes):
            finish(mix)
            total_ref[rows, :] = jnp.dot(mixed_ref[rows, :], received[...], preferred_element_type=F32)
        finish(rest)
        for rows in every:
            dmat = dmat_ref[rows, :]
            fresh = scale_rows(old_own_ref[rows, :].astype(F32) + total_ref[rows, :], dmat).astype(BF16)
            features_ref[rows, :] = fresh[:, :split]
            embeddings_ref[rows, :] = fresh[:, split:]
            z_ref[rows, :] = scale_rows(fresh.astype(F32), dmat).astype(BF16)
        writes += copies.start(
            (features_ref, all_features.at[hop - 1]), (embeddings_ref, all_embeddings.at[hop - 1])
        )
    finish(late + tables)
    for b, rows in enumerate(every):
        columns = [columns_ref[k, b] for k in range(per_block)]
        tiles = [tiles_ref[b, k] for k in range(per_block)]
        values = jnp.concatenate(
            [jnp.where(c < blocks, t, jnp.zeros_like(t)) for c, t in zip(columns, tiles)], axis=1
        )
        picked = jnp.concatenate([z_ref[block_rows(jnp.minimum(c, blocks - 1), tile), :] for c in columns], axis=0)
        own_ref[rows, :] = jnp.dot(values, picked, preferred_element_type=F32).astype(BF16)
        if b % 2:
            pair = slice((b - 1) * tile, (b + 1) * tile)
            writes += copies.start((own_ref.at[pair, :], own_hbm.at[pair, :]))
        if first:
            for slot in range(rim):
                total = jnp.zeros((tile, tile), F32)
                for c, t in zip(columns, tiles):
                    total += jnp.where(c == blocks + slot, t, jnp.zeros_like(t)).astype(F32)
                mixed_ref[rows, slot * tile : (slot + 1) * tile] = total.astype(BF16)
            mixed_ref[rows, rim * tile :] = weight_ref[:, rows].astype(F32).T.astype(BF16)
    if blocks % 2:
        writes += copies.start((own_ref.at[every[-1], :], own_hbm.at[every[-1], :]))
    if first:
        writes += copies.start((mixed_ref, mixed_out), (dmat_ref, dmat_out))
    if not last:
        listed = slots(blocks_ref, count_ref)
        gather_sent(own_ref, own_sent, listed, hubs_ref)
    if first:
        gather_sent(mixed_ref, mixed_sent, listed, hubs_ref)
        gather_roots(degree_ref, roots_sent, listed, hubs_ref)
    finish(writes)


def edge_kernel(
    own_ref, mixed_ref, roots_ref, from_chip_ref, from_core_ref, gathered_ref,
    chip_ref, core_ref, spread_hbm, received_hbm,
    total_ref, received, spread_ref, sems,
):
    copies = Copies(sems)
    rim_rows = chip_ref.shape[0]
    hub_dev = spread_ref.shape[1]
    place_received(from_chip_ref, from_core_ref, gathered_ref, received)
    writes = copies.start((received, received_hbm))
    total_ref[...] = jnp.dot(mixed_ref[...], received[...], preferred_element_type=F32)

    tile = roots_ref.shape[1]

    def fresh(part):
        rows = slice(part * tile, min((part + 1) * tile, total_ref.shape[0]))
        dmat = lane_to_rows(roots_ref[part : part + 1, :])[: rows.stop - rows.start]
        kept = scale_rows(own_ref[rows, :].astype(F32) + total_ref[rows, :], dmat).astype(BF16)
        return scale_rows(kept.astype(F32), dmat).astype(BF16)

    send_most = rim_rows // tile
    hub = fresh(2 * send_most)
    writes += spread_rows(hub[:hub_dev], spread_ref, spread_hbm, copies)
    for slot in range(send_most):
        chip_ref[slot * tile : (slot + 1) * tile, :] = fresh(slot)
        core_ref[slot * tile : (slot + 1) * tile, :] = fresh(send_most + slot)
    finish(writes)


def final_kernel(
    own_hbm, mixed_ref, dmat_ref, from_chip_ref, from_core_ref, gathered_ref, _, __,
    all_features, all_embeddings,
    own_ref, total_ref, features_ref, embeddings_ref, received, sems,
):
    copies = Copies(sems)
    split = features_ref.shape[1]
    row_count = own_ref.shape[0]
    reads = copies.start((own_hbm, own_ref))
    place_received(from_chip_ref, from_core_ref, gathered_ref, received)
    parts = quarters(row_count)

    def multiply(rows):
        total_ref[rows, :] = jnp.dot(mixed_ref[rows, :], received[...], preferred_element_type=F32)

    def store(rows):
        fresh = scale_rows(own_ref[rows, :].astype(F32) + total_ref[rows, :], dmat_ref[rows, :]).astype(BF16)
        features_ref[rows, :] = fresh[:, :split]
        embeddings_ref[rows, :] = fresh[:, split:]
        return copies.start(
            (features_ref.at[rows, :], all_features.at[HOPS - 1, rows, :]),
            (embeddings_ref.at[rows, :], all_embeddings.at[HOPS - 1, rows, :]),
        )

    multiply(parts[0])
    multiply(parts[1])
    finish(reads)
    writes = store(parts[0])
    multiply(parts[2])
    writes += store(parts[1])
    multiply(parts[3])
    writes += store(parts[2])
    writes += store(parts[3])
    finish(writes)


def body(
    features, embeddings, tile_values, tile_columns, send_blocks, send_count, hub_rows, hub_weight, degree,
):
    row_count, split = features.shape
    blocks, per_block, tile, _ = tile_values.shape
    extra = embeddings.shape[1]
    width = split + extra
    send_most = send_blocks.shape[2]
    hub_dev = hub_rows.shape[0]
    hub_total = hub_weight.shape[1]
    count = lax.axis_size("dom")
    rim = 2 * send_most
    deep = rim * tile + hub_total
    sent = rim * tile + GROUP

    vmem = pl.BlockSpec(memory_space=VMEM)
    hbm = pl.BlockSpec(memory_space=pltpu.HBM)
    shape = jax.ShapeDtypeStruct
    int32 = jnp.int32

    def pin(*values):
        return [pltpu.with_memory_space_constraint(value, pltpu.HBM) for value in values]

    def call(kernel, name, flops, out_shape, scratch, sems, in_hbm, operands, aliases={}):
        specs = [hbm] * in_hbm + [vmem] * (len(operands) - in_hbm)
        for source, target in aliases.items():
            if not isinstance(out_shape[target], shape):
                specs[source] = hbm
        return pl.pallas_call(
            kernel,
            name=name,
            out_shape=out_shape,
            in_specs=specs,
            out_specs=[vmem if isinstance(out, shape) else hbm for out in out_shape],
            scratch_shapes=scratch + [pltpu.SemaphoreType.DMA((sems,))],
            input_output_aliases=aliases,
            compiler_params=pltpu.CompilerParams(vmem_limit_bytes=32 * 2**20),
            cost_estimate=pl.CostEstimate(flops=flops, bytes_accessed=0, transcendentals=0),
        )(*operands)

    tables = [SMEM(send_blocks.shape, int32), SMEM(send_count.shape, int32), SMEM(hub_rows.shape, int32)]
    sends = [
        shape((send_most * tile, width), BF16), shape((send_most * tile, width), BF16),
        pltpu.HBM((count, hub_dev, width), BF16),
    ]
    spread_buffer = VMEM((count, hub_dev, width), BF16)
    whole = [pltpu.HBM((HOPS, row_count, split), BF16), pltpu.HBM((HOPS, row_count, extra), BF16)]
    row_buffers = [VMEM((row_count, split), BF16), VMEM((row_count, extra), BF16)]
    lists = pin(send_blocks, send_count, hub_rows)
    rows = pin(degree.reshape(blocks, tile), features, embeddings)
    to_chip, to_core, spread = call(
        prologue_kernel, "prologue", 10**8, sends,
        tables + [VMEM((blocks, tile), int32)] + row_buffers + [spread_buffer], 7, 6, lists + rows,
    )

    core_pairs = [(i, i ^ 1) for i in range(count) if i ^ 1 < count]
    chip_pairs = [p for i in range(1, count - 1, 2) for p in ((i, i + 1), (i + 1, i))]
    fixed = lists + pin(tile_columns.T, tile_values)
    out = []
    for hop in range(HOPS):
        first, last = hop == 0, hop == HOPS - 1
        from_chip = lax.ppermute(to_chip, "dom", chip_pairs)
        from_core = lax.ppermute(to_core, "dom", core_pairs)
        gathered = lax.all_to_all(spread, "dom", 0, 0).reshape(hub_total, width)

        scratch = tables + [
            SMEM((per_block, blocks), int32), VMEM(tile_values.shape, BF16), VMEM((row_count, width), BF16),
            VMEM((row_count, width), BF16),
        ] + row_buffers
        if not last:
            scratch += [VMEM((row_count, deep), BF16), VMEM((row_count, tile), F32)]
        aliases = {}
        full_own = pltpu.HBM((row_count, width), BF16)
        sent_shapes = [shape((sent, width), BF16), shape((sent, deep), BF16)]
        if first:
            operands = fixed + rows + pin(hub_weight.T)
            out_shape = [full_own] + sent_shapes + [shape((rim + 1, tile), F32)]
            out_shape[2:2] = [pltpu.HBM((row_count, deep), BF16), pltpu.HBM((row_count, tile), F32)]
            scratch += [VMEM((blocks, tile), int32), VMEM((hub_total, row_count), BF16)]
        else:
            operands = fixed + pin(own, mixed, dmat, received)
            if out:
                aliases = {len(operands): 0, len(operands) + 1: 1}
                operands += pin(*out)
            out_shape = whole + [full_own]
            out_shape += [shape((row_count, deep), BF16), shape((row_count, tile), F32)] if last else sent_shapes[:1]
            scratch += [VMEM((deep, width), BF16), VMEM((row_count, width), BF16), VMEM((row_count, width), F32)]
        got = call(
            functools.partial(bulk_kernel, hop=hop, rim=rim, per_block=per_block), f"bulk{hop}",
            4 * row_count * per_block * tile * width, out_shape, scratch, 16 + blocks,
            len(operands), operands, aliases,
        )
        if first:
            own, own_sent, mixed, dmat, mixed_sent, roots_sent = got
        else:
            out, (own, *got) = got[:2], got[2:]
            if last:
                mixed_here, dmat_here = got
            else:
                (own_sent,) = got

        flops = 2 * row_count * deep * width
        if last:
            operands = pin(own) + [mixed_here, dmat_here, from_chip, from_core, gathered]
            aliases = {len(operands): 0, len(operands) + 1: 1}
            out = call(
                final_kernel, "final", flops, whole,
                [VMEM((row_count, width), BF16), VMEM((row_count, width), F32)] + row_buffers
                + [VMEM((deep, width), BF16)], 9,
                1, operands + pin(*out), aliases,
            )
        else:
            to_chip, to_core, spread, received = call(
                edge_kernel, f"edge{hop}", flops, sends + [pltpu.HBM((deep, width), BF16)],
                [VMEM((sent, width), F32), VMEM((deep, width), BF16), spread_buffer], 2,
                0, [own_sent, mixed_sent, roots_sent, from_chip, from_core, gathered],
                {3: 0, 4: 1},
            )
    return out[0], out[1]


def solution(mesh):
    placed = (
        P("dom", None),
        P("dom", None),
        P("dom", None, None, None),
        P("dom", None),
        P("dom", None, None),
        P("dom", None),
        P("dom"),
        P("dom", None),
        P("dom"),
    )
    return jax.shard_map(
        body,
        mesh=mesh,
        in_specs=placed,
        out_specs=(P(None, "dom", None), P(None, "dom", None)),
        check_vma=False,
    )
```

```python
import functools

import jax
import jax.numpy as jnp
from jax import lax
from jax.experimental import pallas as pl
from jax.experimental.pallas import tpu as pltpu
from jax.sharding import PartitionSpec as P

HOPS = 3
VMEM = pltpu.VMEM
SMEM = pltpu.SMEM
BF16 = jnp.bfloat16
F32 = jnp.float32
GROUP = 16


def scale_rows(value, dmat):
    lanes = dmat.shape[1]
    pieces = [value[:, i : i + lanes] * dmat for i in range(0, value.shape[1], lanes)]
    return pieces[0] if len(pieces) == 1 else jnp.concatenate(pieces, axis=1)


def finish(copies):
    for copy in copies:
        copy.wait()


class Copies:
    def __init__(self, sems):
        self.sems, self.used = sems, 0

    def start(self, *pairs):
        begun = []
        for source, target in pairs:
            copy = pltpu.make_async_copy(source, target, self.sems.at[self.used])
            copy.start()
            begun.append(copy)
            self.used += 1
        return begun


def block_rows(index, tile):
    return pl.ds(pl.multiple_of(index * tile, tile), tile)


def one_row(ref, row):
    base = pl.multiple_of(row // GROUP * GROUP, GROUP)
    near = ref[pl.ds(base, GROUP), :].astype(F32)
    at = lax.broadcasted_iota(jnp.int32, near.shape, 0) == row % GROUP
    return jnp.sum(jnp.where(at, near, 0.0), axis=0, keepdims=True)


def lane_to_rows(root):
    return jnp.broadcast_to(root, (root.shape[1], root.shape[1])).T


def roots_of(degree_ref, index):
    return lax.rsqrt(degree_ref[pl.ds(index, 1), :].astype(F32))


def factor_block(degree_ref, index):
    return lane_to_rows(roots_of(degree_ref, index))


def hub_roots(degree_ref, hubs_ref):
    tile = degree_ref.shape[1]
    found = []
    for i in range(hubs_ref.shape[0]):
        roots = roots_of(degree_ref, hubs_ref[i] // tile)
        at = lax.broadcasted_iota(jnp.int32, roots.shape, 1) == hubs_ref[i] % tile
        found.append(jnp.sum(jnp.where(at, roots, 0.0), axis=1, keepdims=True))
    return found


def gather_roots(degree_ref, roots_ref, listed, hubs_ref):
    tile = degree_ref.shape[1]
    rows = [roots_of(degree_ref, index) for index, _ in listed]
    lane = lax.broadcasted_iota(jnp.int32, (1, tile), 1)
    last = jnp.zeros((1, tile), F32)
    for i, root in enumerate(hub_roots(degree_ref, hubs_ref)):
        last = jnp.where(lane == i, jnp.broadcast_to(root, (1, tile)), last)
    roots_ref[...] = jnp.concatenate(rows + [last], axis=0)


def quarters(row_count):
    part = row_count // 4
    return [slice(i, i + part) for i in range(0, row_count, part)]


def slots(blocks_ref, count_ref):
    parity = lax.axis_index("dom") % 2
    send_most = blocks_ref.shape[2]
    return [
        (blocks_ref[0, side, slot], slot < count_ref[0, side])
        for side in (parity, 1 - parity)
        for slot in range(send_most)
    ]


def gather_sent(source_ref, target_ref, listed, hubs_ref):
    tile = (target_ref.shape[0] - GROUP) // len(listed)
    width = source_ref.shape[1]
    for i, (index, live) in enumerate(listed):
        block = source_ref[block_rows(index, tile), :]
        target_ref[i * tile : (i + 1) * tile, :] = jnp.where(live, block, jnp.zeros_like(block))
    rows = [one_row(source_ref, hubs_ref[i]) for i in range(hubs_ref.shape[0])]
    rows.append(jnp.zeros((GROUP - len(rows), width), F32))
    target_ref[len(listed) * tile :, :] = jnp.concatenate(rows, axis=0).astype(target_ref.dtype)


def place_received(from_chip_ref, from_core_ref, gathered_ref, received):
    rim_rows = from_chip_ref.shape[0]
    parity = lax.axis_index("dom") % 2
    received[block_rows(parity, rim_rows), :] = from_chip_ref[...]
    received[block_rows(1 - parity, rim_rows), :] = from_core_ref[...]
    received[2 * rim_rows :, :] = gathered_ref[...]


def spread_rows(rows, spread_ref, spread_hbm, copies):
    spread_ref[...] = jnp.broadcast_to(rows[None], spread_ref.shape)
    return copies.start((spread_ref, spread_hbm))


def prologue_kernel(
    blocks_hbm, count_hbm, hubs_hbm, degree_hbm, features_hbm, embeddings_hbm,
    chip_ref, core_ref, spread_hbm,
    blocks_ref, count_ref, hubs_ref, degree_ref, features_ref, embeddings_ref, spread_ref, sems,
):
    copies = Copies(sems)
    tile = degree_ref.shape[1]
    split = features_ref.shape[1]
    tables = copies.start(
        (blocks_hbm, blocks_ref), (count_hbm, count_ref), (hubs_hbm, hubs_ref), (degree_hbm, degree_ref)
    )
    rows = copies.start((features_hbm, features_ref), (embeddings_hbm, embeddings_ref))
    finish(tables)
    listed = slots(blocks_ref, count_ref)
    factors = [factor_block(degree_ref, index) for index, _ in listed]
    finish(rows)
    hubs = []
    for i, root in enumerate(hub_roots(degree_ref, hubs_ref)):
        row = hubs_ref[i]
        whole = jnp.concatenate([one_row(features_ref, row), one_row(embeddings_ref, row)], axis=1)
        hubs.append(scale_rows(whole, jnp.broadcast_to(root, (1, tile))))
    writes = spread_rows(jnp.concatenate(hubs, axis=0).astype(BF16), spread_ref, spread_hbm, copies)
    half = len(listed) // 2
    for i, (index, live) in enumerate(listed):
        target = (chip_ref, core_ref)[i // half]
        into = slice((i % half) * tile, (i % half + 1) * tile)
        for source, columns in ((features_ref, slice(0, split)), (embeddings_ref, slice(split, None))):
            block = scale_rows(source[block_rows(index, tile), :].astype(F32), factors[i])
            target[into, columns] = jnp.where(live, block, 0.0).astype(BF16)
    finish(writes)


def bulk_kernel(*refs, hop, rim, per_block):
    refs = list(refs)
    take = lambda n: [refs.pop(0) for _ in range(n)]
    blocks_hbm, count_hbm, hubs_hbm, columns_hbm, tiles_hbm = take(5)
    first, last = hop == 0, hop == HOPS - 1
    if first:
        degree_hbm, features_hbm, embeddings_hbm, weight_hbm = take(4)
        own_hbm, own_sent, mixed_out, dmat_out, mixed_sent, roots_sent = take(6)
    else:
        old_own_hbm, mixed_hbm, dmat_hbm, received_hbm = take(4)
        if hop > 1:
            take(2)
        all_features, all_embeddings, own_hbm = take(3)
        if last:
            mixed_ref, dmat_ref = take(2)
        else:
            (own_sent,) = take(1)
    blocks_ref, count_ref, hubs_ref, columns_ref = take(4)
    tiles_ref, z_ref, own_ref, features_ref, embeddings_ref = take(5)
    if not last:
        mixed_ref, dmat_ref = take(2)
    if first:
        degree_ref, weight_ref, sems = refs
    else:
        received, old_own_ref, sems = refs
    copies = Copies(sems)
    blocks, _, tile, _ = tiles_ref.shape
    row_count, width = z_ref.shape
    split = features_ref.shape[1]
    every = [slice(b * tile, (b + 1) * tile) for b in range(blocks)]

    tables = copies.start((columns_hbm, columns_ref))
    if not last:
        tables += copies.start((blocks_hbm, blocks_ref), (count_hbm, count_ref), (hubs_hbm, hubs_ref))
    writes = []
    if first:
        finish(copies.start((degree_hbm, degree_ref), (features_hbm, features_ref),
                            (embeddings_hbm, embeddings_ref)))
        late = copies.start((tiles_hbm, tiles_ref), (weight_hbm, weight_ref))
        for b, rows in enumerate(every):
            dmat = factor_block(degree_ref, b)
            dmat_ref[rows, :] = dmat
            z_ref[rows, :split] = scale_rows(features_ref[rows, :].astype(F32), dmat).astype(BF16)
            z_ref[rows, split:] = scale_rows(embeddings_ref[rows, :].astype(F32), dmat).astype(BF16)
    else:
        inputs = copies.start((received_hbm, received), (dmat_hbm, dmat_ref))
        parts = [
            copies.start((mixed_hbm.at[rows, :], mixed_ref.at[rows, :]), (old_own_hbm.at[rows, :], old_own_ref.at[rows, :]))
            for rows in quarters(row_count)
        ]
        late = copies.start((tiles_hbm, tiles_ref))
        finish(inputs)
        for b, rows in enumerate(every):
            if b * len(parts) % blocks == 0:
                finish(parts[b * len(parts) // blocks])
            total = jnp.dot(mixed_ref[rows, :], received[...], preferred_element_type=F32)
            dmat = dmat_ref[rows, :]
            fresh = scale_rows(old_own_ref[rows, :].astype(F32) + total, dmat).astype(BF16)
            features_ref[rows, :] = fresh[:, :split]
            embeddings_ref[rows, :] = fresh[:, split:]
            z_ref[rows, :] = scale_rows(fresh.astype(F32), dmat).astype(BF16)
        writes += copies.start(
            (features_ref, all_features.at[hop - 1]), (embeddings_ref, all_embeddings.at[hop - 1])
        )
    finish(late + tables)
    for b, rows in enumerate(every):
        columns = [columns_ref[k, b] for k in range(per_block)]
        tiles = [tiles_ref[b, k] for k in range(per_block)]
        values = jnp.concatenate(
            [jnp.where(c < blocks, t, jnp.zeros_like(t)) for c, t in zip(columns, tiles)], axis=1
        )
        picked = jnp.concatenate([z_ref[block_rows(jnp.minimum(c, blocks - 1), tile), :] for c in columns], axis=0)
        own_ref[rows, :] = jnp.dot(values, picked, preferred_element_type=F32).astype(BF16)
        if b % 2:
            pair = slice((b - 1) * tile, (b + 1) * tile)
            writes += copies.start((own_ref.at[pair, :], own_hbm.at[pair, :]))
        if first:
            for slot in range(rim):
                total = jnp.zeros((tile, tile), F32)
                for c, t in zip(columns, tiles):
                    total += jnp.where(c == blocks + slot, t, jnp.zeros_like(t)).astype(F32)
                mixed_ref[rows, slot * tile : (slot + 1) * tile] = total.astype(BF16)
            mixed_ref[rows, rim * tile :] = weight_ref[:, rows].astype(F32).T.astype(BF16)
    if blocks % 2:
        writes += copies.start((own_ref.at[every[-1], :], own_hbm.at[every[-1], :]))
    if first:
        writes += copies.start((mixed_ref, mixed_out), (dmat_ref, dmat_out))
    if not last:
        listed = slots(blocks_ref, count_ref)
        gather_sent(own_ref, own_sent, listed, hubs_ref)
    if first:
        gather_sent(mixed_ref, mixed_sent, listed, hubs_ref)
        gather_roots(degree_ref, roots_sent, listed, hubs_ref)
    finish(writes)


def edge_kernel(
    own_ref, mixed_ref, roots_ref, from_chip_ref, from_core_ref, gathered_ref,
    chip_ref, core_ref, spread_hbm, received_hbm,
    received, spread_ref, sems,
):
    copies = Copies(sems)
    rim_rows = chip_ref.shape[0]
    hub_dev = spread_ref.shape[1]
    place_received(from_chip_ref, from_core_ref, gathered_ref, received)
    writes = copies.start((received, received_hbm))
    tile = roots_ref.shape[1]

    def fresh(part):
        rows = slice(part * tile, min((part + 1) * tile, own_ref.shape[0]))
        total = jnp.dot(mixed_ref[rows, :], received[...], preferred_element_type=F32)
        dmat = lane_to_rows(roots_ref[part : part + 1, :])[: rows.stop - rows.start]
        kept = scale_rows(own_ref[rows, :].astype(F32) + total, dmat).astype(BF16)
        return scale_rows(kept.astype(F32), dmat).astype(BF16)

    send_most = rim_rows // tile
    hub = fresh(2 * send_most)
    writes += spread_rows(hub[:hub_dev], spread_ref, spread_hbm, copies)
    for slot in range(send_most):
        chip_ref[slot * tile : (slot + 1) * tile, :] = fresh(slot)
        core_ref[slot * tile : (slot + 1) * tile, :] = fresh(send_most + slot)
    finish(writes)


def final_kernel(
    own_hbm, mixed_ref, dmat_ref, from_chip_ref, from_core_ref, gathered_ref, _, __,
    all_features, all_embeddings,
    own_ref, total_ref, features_ref, embeddings_ref, received, sems,
):
    copies = Copies(sems)
    split = features_ref.shape[1]
    row_count = own_ref.shape[0]
    reads = copies.start((own_hbm, own_ref))
    place_received(from_chip_ref, from_core_ref, gathered_ref, received)
    tile = dmat_ref.shape[1]
    parts = [slice(at, at + tile) for at in range(0, row_count, tile)]
    ahead = len(parts) // 2
    for rows in parts[:ahead]:
        total_ref[rows, :] = jnp.dot(mixed_ref[rows, :], received[...], preferred_element_type=F32)
    finish(reads)
    writes = []
    for i, rows in enumerate(parts):
        if i < ahead:
            total = total_ref[rows, :]
        else:
            total = jnp.dot(mixed_ref[rows, :], received[...], preferred_element_type=F32)
        fresh = scale_rows(own_ref[rows, :].astype(F32) + total, dmat_ref[rows, :]).astype(BF16)
        features_ref[rows, :] = fresh[:, :split]
        embeddings_ref[rows, :] = fresh[:, split:]
        writes += copies.start(
            (features_ref.at[rows, :], all_features.at[HOPS - 1, rows, :]),
            (embeddings_ref.at[rows, :], all_embeddings.at[HOPS - 1, rows, :]),
        )
    finish(writes)


def body(
    features, embeddings, tile_values, tile_columns, send_blocks, send_count, hub_rows, hub_weight, degree,
):
    row_count, split = features.shape
    blocks, per_block, tile, _ = tile_values.shape
    extra = embeddings.shape[1]
    width = split + extra
    send_most = send_blocks.shape[2]
    hub_dev = hub_rows.shape[0]
    hub_total = hub_weight.shape[1]
    count = lax.axis_size("dom")
    rim = 2 * send_most
    deep = rim * tile + hub_total
    sent = rim * tile + GROUP

    vmem = pl.BlockSpec(memory_space=VMEM)
    hbm = pl.BlockSpec(memory_space=pltpu.HBM)
    shape = jax.ShapeDtypeStruct
    int32 = jnp.int32

    def pin(*values):
        return [pltpu.with_memory_space_constraint(value, pltpu.HBM) for value in values]

    def call(kernel, name, flops, out_shape, scratch, sems, in_hbm, operands, aliases={}):
        specs = [hbm] * in_hbm + [vmem] * (len(operands) - in_hbm)
        for source, target in aliases.items():
            if not isinstance(out_shape[target], shape):
                specs[source] = hbm
        return pl.pallas_call(
            kernel,
            name=name,
            out_shape=out_shape,
            in_specs=specs,
            out_specs=[vmem if isinstance(out, shape) else hbm for out in out_shape],
            scratch_shapes=scratch + [pltpu.SemaphoreType.DMA((sems,))],
            input_output_aliases=aliases,
            compiler_params=pltpu.CompilerParams(vmem_limit_bytes=32 * 2**20),
            cost_estimate=pl.CostEstimate(flops=flops, bytes_accessed=0, transcendentals=0),
        )(*operands)

    tables = [SMEM(send_blocks.shape, int32), SMEM(send_count.shape, int32), SMEM(hub_rows.shape, int32)]
    sends = [
        shape((send_most * tile, width), BF16), shape((send_most * tile, width), BF16),
        pltpu.HBM((count, hub_dev, width), BF16),
    ]
    spread_buffer = VMEM((count, hub_dev, width), BF16)
    whole = [pltpu.HBM((HOPS, row_count, split), BF16), pltpu.HBM((HOPS, row_count, extra), BF16)]
    row_buffers = [VMEM((row_count, split), BF16), VMEM((row_count, extra), BF16)]
    lists = pin(send_blocks, send_count, hub_rows)
    rows = pin(degree.reshape(blocks, tile), features, embeddings)
    to_chip, to_core, spread = call(
        prologue_kernel, "prologue", 10**8, sends,
        tables + [VMEM((blocks, tile), int32)] + row_buffers + [spread_buffer], 7, 6, lists + rows,
    )

    core_pairs = [(i, i ^ 1) for i in range(count) if i ^ 1 < count]
    chip_pairs = [p for i in range(1, count - 1, 2) for p in ((i, i + 1), (i + 1, i))]
    fixed = lists + pin(tile_columns.T, tile_values)
    out = []
    for hop in range(HOPS):
        first, last = hop == 0, hop == HOPS - 1
        from_chip = lax.ppermute(to_chip, "dom", chip_pairs)
        from_core = lax.ppermute(to_core, "dom", core_pairs)
        gathered = lax.all_to_all(spread, "dom", 0, 0).reshape(hub_total, width)

        scratch = tables + [
            SMEM((per_block, blocks), int32), VMEM(tile_values.shape, BF16), VMEM((row_count, width), BF16),
            VMEM((row_count, width), BF16),
        ] + row_buffers
        if not last:
            scratch += [VMEM((row_count, deep), BF16), VMEM((row_count, tile), F32)]
        aliases = {}
        full_own = pltpu.HBM((row_count, width), BF16)
        sent_shapes = [shape((sent, width), BF16), shape((sent, deep), BF16)]
        if first:
            operands = fixed + rows + pin(hub_weight.T)
            out_shape = [full_own] + sent_shapes + [shape((rim + 1, tile), F32)]
            out_shape[2:2] = [pltpu.HBM((row_count, deep), BF16), pltpu.HBM((row_count, tile), F32)]
            scratch += [VMEM((blocks, tile), int32), VMEM((hub_total, row_count), BF16)]
        else:
            operands = fixed + pin(own, mixed, dmat, received)
            if out:
                aliases = {len(operands): 0, len(operands) + 1: 1}
                operands += pin(*out)
            out_shape = whole + [full_own]
            out_shape += [shape((row_count, deep), BF16), shape((row_count, tile), F32)] if last else sent_shapes[:1]
            scratch += [VMEM((deep, width), BF16), VMEM((row_count, width), BF16)]
        got = call(
            functools.partial(bulk_kernel, hop=hop, rim=rim, per_block=per_block), f"bulk{hop}",
            4 * row_count * per_block * tile * width, out_shape, scratch, 20 + blocks,
            len(operands), operands, aliases,
        )
        if first:
            own, own_sent, mixed, dmat, mixed_sent, roots_sent = got
        else:
            out, (own, *got) = got[:2], got[2:]
            if last:
                mixed_here, dmat_here = got
            else:
                (own_sent,) = got

        flops = 2 * row_count * deep * width
        if last:
            operands = pin(own) + [mixed_here, dmat_here, from_chip, from_core, gathered]
            aliases = {len(operands): 0, len(operands) + 1: 1}
            out = call(
                final_kernel, "final", flops, whole,
                [VMEM((row_count, width), BF16), VMEM((row_count, width), F32)] + row_buffers
                + [VMEM((deep, width), BF16)], 1 + 2 * blocks,
                1, operands + pin(*out), aliases,
            )
        else:
            to_chip, to_core, spread, received = call(
                edge_kernel, f"edge{hop}", flops, sends + [pltpu.HBM((deep, width), BF16)],
                [VMEM((deep, width), BF16), spread_buffer], 2,
                0, [own_sent, mixed_sent, roots_sent, from_chip, from_core, gathered],
                {3: 0, 4: 1},
            )
    return out[0], out[1]


def solution(mesh):
    placed = (
        P("dom", None),
        P("dom", None),
        P("dom", None, None, None),
        P("dom", None),
        P("dom", None, None),
        P("dom", None),
        P("dom"),
        P("dom", None),
        P("dom"),
    )
    return jax.shard_map(
        body,
        mesh=mesh,
        in_specs=placed,
        out_specs=(P(None, "dom", None), P(None, "dom", None)),
        check_vma=False,
    )
```

```python
import functools

import jax
import jax.numpy as jnp
from jax import lax
from jax.experimental import pallas as pl
from jax.experimental.pallas import tpu as pltpu
from jax.sharding import PartitionSpec as P

HOPS = 3
VMEM = pltpu.VMEM
SMEM = pltpu.SMEM
BF16 = jnp.bfloat16
F32 = jnp.float32
GROUP = 16


def scale_rows(value, dmat):
    lanes = dmat.shape[1]
    pieces = [value[:, i : i + lanes] * dmat for i in range(0, value.shape[1], lanes)]
    return pieces[0] if len(pieces) == 1 else jnp.concatenate(pieces, axis=1)


def finish(copies):
    for copy in copies:
        copy.wait()


class Copies:
    def __init__(self, sems):
        self.sems, self.used = sems, 0

    def start(self, *pairs):
        begun = []
        for source, target in pairs:
            copy = pltpu.make_async_copy(source, target, self.sems.at[self.used])
            copy.start()
            begun.append(copy)
            self.used += 1
        return begun


def block_rows(index, tile):
    return pl.ds(pl.multiple_of(index * tile, tile), tile)


def one_row(ref, row):
    base = pl.multiple_of(row // GROUP * GROUP, GROUP)
    near = ref[pl.ds(base, GROUP), :].astype(F32)
    at = lax.broadcasted_iota(jnp.int32, near.shape, 0) == row % GROUP
    return jnp.sum(jnp.where(at, near, 0.0), axis=0, keepdims=True)


def lane_to_rows(root):
    return jnp.broadcast_to(root, (root.shape[1], root.shape[1])).T


def roots_of(degree_ref, index):
    return lax.rsqrt(degree_ref[pl.ds(index, 1), :].astype(F32))


def factor_block(degree_ref, index):
    return lane_to_rows(roots_of(degree_ref, index))


def hub_roots(degree_ref, hubs_ref):
    tile = degree_ref.shape[1]
    found = []
    for i in range(hubs_ref.shape[0]):
        roots = roots_of(degree_ref, hubs_ref[i] // tile)
        at = lax.broadcasted_iota(jnp.int32, roots.shape, 1) == hubs_ref[i] % tile
        found.append(jnp.sum(jnp.where(at, roots, 0.0), axis=1, keepdims=True))
    return found


def gather_roots(degree_ref, roots_ref, listed, hubs_ref):
    tile = degree_ref.shape[1]
    rows = [roots_of(degree_ref, index) for index, _ in listed]
    lane = lax.broadcasted_iota(jnp.int32, (1, tile), 1)
    last = jnp.zeros((1, tile), F32)
    for i, root in enumerate(hub_roots(degree_ref, hubs_ref)):
        last = jnp.where(lane == i, jnp.broadcast_to(root, (1, tile)), last)
    roots_ref[...] = jnp.concatenate(rows + [last], axis=0)


def quarters(row_count):
    part = row_count // 4
    return [slice(i, i + part) for i in range(0, row_count, part)]


def slots(blocks_ref, count_ref):
    index = lax.axis_index("dom")
    parity = index % 2
    send_most = blocks_ref.shape[2]
    inner = jnp.logical_and(index > 0, index < lax.axis_size("dom") - 1)
    return [
        (blocks_ref[0, side, slot], jnp.logical_and(slot < count_ref[0, side], real))
        for side, real in ((parity, inner), (1 - parity, True))
        for slot in range(send_most)
    ]


def gather_sent(source_ref, target_ref, listed, hubs_ref):
    tile = (target_ref.shape[0] - GROUP) // len(listed)
    width = source_ref.shape[1]
    for i, (index, live) in enumerate(listed):
        block = source_ref[block_rows(index, tile), :]
        target_ref[i * tile : (i + 1) * tile, :] = jnp.where(live, block, jnp.zeros_like(block))
    rows = [one_row(source_ref, hubs_ref[i]) for i in range(hubs_ref.shape[0])]
    rows.append(jnp.zeros((GROUP - len(rows), width), F32))
    target_ref[len(listed) * tile :, :] = jnp.concatenate(rows, axis=0).astype(target_ref.dtype)


def place_received(from_chip_ref, from_core_ref, gathered_ref, received):
    rim_rows = from_chip_ref.shape[0]
    parity = lax.axis_index("dom") % 2
    received[block_rows(parity, rim_rows), :] = from_chip_ref[...]
    received[block_rows(1 - parity, rim_rows), :] = from_core_ref[...]
    received[2 * rim_rows :, :] = gathered_ref[...]


def spread_rows(rows, spread_ref, spread_hbm, copies):
    spread_ref[...] = jnp.broadcast_to(rows[None], spread_ref.shape)
    return copies.start((spread_ref, spread_hbm))


def prologue_kernel(
    blocks_hbm, count_hbm, hubs_hbm, degree_hbm, features_hbm, embeddings_hbm,
    chip_ref, core_ref, spread_hbm,
    blocks_ref, count_ref, hubs_ref, degree_ref, features_ref, embeddings_ref, spread_ref, sems,
):
    copies = Copies(sems)
    tile = degree_ref.shape[1]
    split = features_ref.shape[1]
    tables = copies.start(
        (blocks_hbm, blocks_ref), (count_hbm, count_ref), (hubs_hbm, hubs_ref), (degree_hbm, degree_ref)
    )
    rows = copies.start((features_hbm, features_ref), (embeddings_hbm, embeddings_ref))
    finish(tables)
    listed = slots(blocks_ref, count_ref)
    factors = [factor_block(degree_ref, index) for index, _ in listed]
    finish(rows)
    hubs = []
    for i, root in enumerate(hub_roots(degree_ref, hubs_ref)):
        row = hubs_ref[i]
        whole = jnp.concatenate([one_row(features_ref, row), one_row(embeddings_ref, row)], axis=1)
        hubs.append(scale_rows(whole, jnp.broadcast_to(root, (1, tile))))
    writes = spread_rows(jnp.concatenate(hubs, axis=0).astype(BF16), spread_ref, spread_hbm, copies)
    half = len(listed) // 2
    for i, (index, live) in enumerate(listed):
        target = (chip_ref, core_ref)[i // half]
        into = slice((i % half) * tile, (i % half + 1) * tile)
        for source, columns in ((features_ref, slice(0, split)), (embeddings_ref, slice(split, None))):
            block = scale_rows(source[block_rows(index, tile), :].astype(F32), factors[i])
            target[into, columns] = jnp.where(live, block, 0.0).astype(BF16)
    finish(writes)


def bulk_kernel(*refs, hop, rim, per_block):
    refs = list(refs)
    take = lambda n: [refs.pop(0) for _ in range(n)]
    blocks_hbm, count_hbm, hubs_hbm, columns_hbm, tiles_hbm = take(5)
    first, last = hop == 0, hop == HOPS - 1
    if first:
        degree_hbm, features_hbm, embeddings_hbm, weight_hbm = take(4)
        own_hbm, own_sent, mixed_out, dmat_out, mixed_sent, roots_sent = take(6)
    else:
        old_own_hbm, mixed_hbm, dmat_hbm, received_hbm = take(4)
        if hop > 1:
            take(2)
        all_features, all_embeddings, own_hbm = take(3)
        if last:
            mixed_ref, dmat_ref = take(2)
        else:
            (own_sent,) = take(1)
    blocks_ref, count_ref, hubs_ref, columns_ref = take(4)
    tiles_ref, z_ref, own_ref, features_ref, embeddings_ref = take(5)
    if not last:
        mixed_ref, dmat_ref = take(2)
    if first:
        degree_ref, weight_ref, sems = refs
    else:
        received, old_own_ref, sems = refs
    copies = Copies(sems)
    blocks, _, tile, _ = tiles_ref.shape
    row_count, width = z_ref.shape
    split = features_ref.shape[1]
    every = [slice(b * tile, (b + 1) * tile) for b in range(blocks)]

    tables = copies.start((columns_hbm, columns_ref))
    if not last:
        tables += copies.start((blocks_hbm, blocks_ref), (count_hbm, count_ref), (hubs_hbm, hubs_ref))
    writes = []
    if first:
        finish(copies.start((degree_hbm, degree_ref), (features_hbm, features_ref),
                            (embeddings_hbm, embeddings_ref)))
        late = copies.start((tiles_hbm, tiles_ref), (weight_hbm, weight_ref))
        for b, rows in enumerate(every):
            dmat = factor_block(degree_ref, b)
            dmat_ref[rows, :] = dmat
            z_ref[rows, :split] = scale_rows(features_ref[rows, :].astype(F32), dmat).astype(BF16)
            z_ref[rows, split:] = scale_rows(embeddings_ref[rows, :].astype(F32), dmat).astype(BF16)
    else:
        inputs = copies.start((received_hbm, received), (dmat_hbm, dmat_ref))
        parts = [
            copies.start((mixed_hbm.at[rows, :], mixed_ref.at[rows, :]), (old_own_hbm.at[rows, :], old_own_ref.at[rows, :]))
            for rows in quarters(row_count)
        ]
        late = copies.start((tiles_hbm, tiles_ref))
        finish(inputs)
        for b, rows in enumerate(every):
            if b * len(parts) % blocks == 0:
                finish(parts[b * len(parts) // blocks])
            total = jnp.dot(mixed_ref[rows, :], received[...], preferred_element_type=F32)
            dmat = dmat_ref[rows, :]
            fresh = scale_rows(old_own_ref[rows, :].astype(F32) + total, dmat).astype(BF16)
            features_ref[rows, :] = fresh[:, :split]
            embeddings_ref[rows, :] = fresh[:, split:]
            z_ref[rows, :] = scale_rows(fresh.astype(F32), dmat).astype(BF16)
        writes += copies.start(
            (features_ref, all_features.at[hop - 1]), (embeddings_ref, all_embeddings.at[hop - 1])
        )
    finish(late + tables)
    for b, rows in enumerate(every):
        columns = [columns_ref[k, b] for k in range(per_block)]
        tiles = [tiles_ref[b, k] for k in range(per_block)]
        values = jnp.concatenate(
            [jnp.where(c < blocks, t, jnp.zeros_like(t)) for c, t in zip(columns, tiles)], axis=1
        )
        picked = jnp.concatenate([z_ref[block_rows(jnp.minimum(c, blocks - 1), tile), :] for c in columns], axis=0)
        own_ref[rows, :] = jnp.dot(values, picked, preferred_element_type=F32).astype(BF16)
        if b % 2:
            pair = slice((b - 1) * tile, (b + 1) * tile)
            writes += copies.start((own_ref.at[pair, :], own_hbm.at[pair, :]))
        if first:
            for slot in range(rim):
                total = jnp.zeros((tile, tile), F32)
                for c, t in zip(columns, tiles):
                    total += jnp.where(c == blocks + slot, t, jnp.zeros_like(t)).astype(F32)
                mixed_ref[rows, slot * tile : (slot + 1) * tile] = total.astype(BF16)
            mixed_ref[rows, rim * tile :] = weight_ref[:, rows].astype(F32).T.astype(BF16)
    if blocks % 2:
        writes += copies.start((own_ref.at[every[-1], :], own_hbm.at[every[-1], :]))
    if first:
        writes += copies.start((mixed_ref, mixed_out), (dmat_ref, dmat_out))
    if not last:
        listed = slots(blocks_ref, count_ref)
        gather_sent(own_ref, own_sent, listed, hubs_ref)
    if first:
        gather_sent(mixed_ref, mixed_sent, listed, hubs_ref)
        gather_roots(degree_ref, roots_sent, listed, hubs_ref)
    finish(writes)


def edge_kernel(
    own_ref, mixed_ref, roots_ref, from_chip_ref, from_core_ref, gathered_ref,
    chip_ref, core_ref, spread_hbm, received_hbm,
    received, spread_ref, sems,
):
    copies = Copies(sems)
    rim_rows = chip_ref.shape[0]
    hub_dev = spread_ref.shape[1]
    place_received(from_chip_ref, from_core_ref, gathered_ref, received)
    writes = copies.start((received, received_hbm))
    tile = roots_ref.shape[1]

    def fresh(part):
        rows = slice(part * tile, min((part + 1) * tile, own_ref.shape[0]))
        total = jnp.dot(mixed_ref[rows, :], received[...], preferred_element_type=F32)
        dmat = lane_to_rows(roots_ref[part : part + 1, :])[: rows.stop - rows.start]
        kept = scale_rows(own_ref[rows, :].astype(F32) + total, dmat).astype(BF16)
        return scale_rows(kept.astype(F32), dmat).astype(BF16)

    send_most = rim_rows // tile
    hub = fresh(2 * send_most)
    writes += spread_rows(hub[:hub_dev], spread_ref, spread_hbm, copies)
    for slot in range(send_most):
        chip_ref[slot * tile : (slot + 1) * tile, :] = fresh(slot)
        core_ref[slot * tile : (slot + 1) * tile, :] = fresh(send_most + slot)
    finish(writes)


def final_kernel(
    own_hbm, mixed_ref, dmat_ref, from_chip_ref, from_core_ref, gathered_ref, _, __,
    all_features, all_embeddings,
    own_ref, total_ref, features_ref, embeddings_ref, received, sems,
):
    copies = Copies(sems)
    split = features_ref.shape[1]
    row_count = own_ref.shape[0]
    reads = copies.start((own_hbm, own_ref))
    place_received(from_chip_ref, from_core_ref, gathered_ref, received)
    tile = dmat_ref.shape[1]
    parts = [slice(at, at + tile) for at in range(0, row_count, tile)]
    ahead = len(parts) // 2
    for rows in parts[:ahead]:
        total_ref[rows, :] = jnp.dot(mixed_ref[rows, :], received[...], preferred_element_type=F32)
    finish(reads)
    writes = []
    for i, rows in enumerate(parts):
        if i < ahead:
            total = total_ref[rows, :]
        else:
            total = jnp.dot(mixed_ref[rows, :], received[...], preferred_element_type=F32)
        fresh = scale_rows(own_ref[rows, :].astype(F32) + total, dmat_ref[rows, :]).astype(BF16)
        features_ref[rows, :] = fresh[:, :split]
        embeddings_ref[rows, :] = fresh[:, split:]
        writes += copies.start(
            (features_ref.at[rows, :], all_features.at[HOPS - 1, rows, :]),
            (embeddings_ref.at[rows, :], all_embeddings.at[HOPS - 1, rows, :]),
        )
    finish(writes)


def body(
    features, embeddings, tile_values, tile_columns, send_blocks, send_count, hub_rows, hub_weight, degree,
):
    row_count, split = features.shape
    blocks, per_block, tile, _ = tile_values.shape
    extra = embeddings.shape[1]
    width = split + extra
    send_most = send_blocks.shape[2]
    hub_dev = hub_rows.shape[0]
    hub_total = hub_weight.shape[1]
    count = lax.axis_size("dom")
    rim = 2 * send_most
    deep = rim * tile + hub_total
    sent = rim * tile + GROUP

    vmem = pl.BlockSpec(memory_space=VMEM)
    hbm = pl.BlockSpec(memory_space=pltpu.HBM)
    shape = jax.ShapeDtypeStruct
    int32 = jnp.int32

    def pin(*values):
        return [pltpu.with_memory_space_constraint(value, pltpu.HBM) for value in values]

    def call(kernel, name, flops, out_shape, scratch, sems, in_hbm, operands, aliases={}):
        specs = [hbm] * in_hbm + [vmem] * (len(operands) - in_hbm)
        for source, target in aliases.items():
            if not isinstance(out_shape[target], shape):
                specs[source] = hbm
        return pl.pallas_call(
            kernel,
            name=name,
            out_shape=out_shape,
            in_specs=specs,
            out_specs=[vmem if isinstance(out, shape) else hbm for out in out_shape],
            scratch_shapes=scratch + [pltpu.SemaphoreType.DMA((sems,))],
            input_output_aliases=aliases,
            compiler_params=pltpu.CompilerParams(vmem_limit_bytes=32 * 2**20),
            cost_estimate=pl.CostEstimate(flops=flops, bytes_accessed=0, transcendentals=0),
        )(*operands)

    tables = [SMEM(send_blocks.shape, int32), SMEM(send_count.shape, int32), SMEM(hub_rows.shape, int32)]
    sends = [
        shape((send_most * tile, width), BF16), shape((send_most * tile, width), BF16),
        pltpu.HBM((count, hub_dev, width), BF16),
    ]
    spread_buffer = VMEM((count, hub_dev, width), BF16)
    whole = [pltpu.HBM((HOPS, row_count, split), BF16), pltpu.HBM((HOPS, row_count, extra), BF16)]
    row_buffers = [VMEM((row_count, split), BF16), VMEM((row_count, extra), BF16)]
    lists = pin(send_blocks, send_count, hub_rows)
    rows = pin(degree.reshape(blocks, tile), features, embeddings)
    to_chip, to_core, spread = call(
        prologue_kernel, "prologue", 10**8, sends,
        tables + [VMEM((blocks, tile), int32)] + row_buffers + [spread_buffer], 7, 6, lists + rows,
    )

    core_pairs = [(i, i ^ 1) for i in range(count) if i ^ 1 < count]
    chip_pairs = [p for i in range(1, count, 2) for p in ((i, (i + 1) % count), ((i + 1) % count, i))]
    fixed = lists + pin(tile_columns.T, tile_values)
    out = []
    for hop in range(HOPS):
        first, last = hop == 0, hop == HOPS - 1
        from_chip = lax.ppermute(to_chip, "dom", chip_pairs)
        from_core = lax.ppermute(to_core, "dom", core_pairs)
        gathered = lax.all_to_all(spread, "dom", 0, 0).reshape(hub_total, width)

        scratch = tables + [
            SMEM((per_block, blocks), int32), VMEM(tile_values.shape, BF16), VMEM((row_count, width), BF16),
            VMEM((row_count, width), BF16),
        ] + row_buffers
        if not last:
            scratch += [VMEM((row_count, deep), BF16), VMEM((row_count, tile), F32)]
        aliases = {}
        full_own = pltpu.HBM((row_count, width), BF16)
        sent_shapes = [shape((sent, width), BF16), shape((sent, deep), BF16)]
        if first:
            operands = fixed + rows + pin(hub_weight.T)
            out_shape = [full_own] + sent_shapes + [shape((rim + 1, tile), F32)]
            out_shape[2:2] = [pltpu.HBM((row_count, deep), BF16), pltpu.HBM((row_count, tile), F32)]
            scratch += [VMEM((blocks, tile), int32), VMEM((hub_total, row_count), BF16)]
        else:
            operands = fixed + pin(own, mixed, dmat, received)
            if out:
                aliases = {len(operands): 0, len(operands) + 1: 1}
                operands += pin(*out)
            out_shape = whole + [full_own]
            out_shape += [shape((row_count, deep), BF16), shape((row_count, tile), F32)] if last else sent_shapes[:1]
            scratch += [VMEM((deep, width), BF16), VMEM((row_count, width), BF16)]
        got = call(
            functools.partial(bulk_kernel, hop=hop, rim=rim, per_block=per_block), f"bulk{hop}",
            4 * row_count * per_block * tile * width, out_shape, scratch, 20 + blocks,
            len(operands), operands, aliases,
        )
        if first:
            own, own_sent, mixed, dmat, mixed_sent, roots_sent = got
        else:
            out, (own, *got) = got[:2], got[2:]
            if last:
                mixed_here, dmat_here = got
            else:
                (own_sent,) = got

        flops = 2 * row_count * deep * width
        if last:
            operands = pin(own) + [mixed_here, dmat_here, from_chip, from_core, gathered]
            aliases = {len(operands): 0, len(operands) + 1: 1}
            out = call(
                final_kernel, "final", flops, whole,
                [VMEM((row_count, width), BF16), VMEM((row_count, width), F32)] + row_buffers
                + [VMEM((deep, width), BF16)], 1 + 2 * blocks,
                1, operands + pin(*out), aliases,
            )
        else:
            to_chip, to_core, spread, received = call(
                edge_kernel, f"edge{hop}", flops, sends + [pltpu.HBM((deep, width), BF16)],
                [VMEM((deep, width), BF16), spread_buffer], 2,
                0, [own_sent, mixed_sent, roots_sent, from_chip, from_core, gathered],
                {3: 0, 4: 1},
            )
    return out[0], out[1]


def solution(mesh):
    placed = (
        P("dom", None),
        P("dom", None),
        P("dom", None, None, None),
        P("dom", None),
        P("dom", None, None),
        P("dom", None),
        P("dom"),
        P("dom", None),
        P("dom"),
    )
    return jax.shard_map(
        body,
        mesh=mesh,
        in_specs=placed,
        out_specs=(P(None, "dom", None), P(None, "dom", None)),
        check_vma=False,
    )
```

```python
import functools

import jax
import jax.numpy as jnp
from jax import lax
from jax.experimental import pallas as pl
from jax.experimental.pallas import tpu as pltpu
from jax.sharding import PartitionSpec as P

HOPS = 3
VMEM = pltpu.VMEM
SMEM = pltpu.SMEM
BF16 = jnp.bfloat16
F32 = jnp.float32
GROUP = 16
KEPT = 2


def scale_rows(value, dmat):
    lanes = dmat.shape[1]
    pieces = [value[:, i : i + lanes] * dmat for i in range(0, value.shape[1], lanes)]
    return pieces[0] if len(pieces) == 1 else jnp.concatenate(pieces, axis=1)


def finish(copies):
    for copy in copies:
        copy.wait()


class Copies:
    def __init__(self, sems):
        self.sems, self.used = sems, 0

    def start(self, *pairs):
        begun = []
        for source, target in pairs:
            copy = pltpu.make_async_copy(source, target, self.sems.at[self.used])
            copy.start()
            begun.append(copy)
            self.used += 1
        return begun


def block_rows(index, tile):
    return pl.ds(pl.multiple_of(index * tile, tile), tile)


def one_row(ref, row):
    base = pl.multiple_of(row // GROUP * GROUP, GROUP)
    near = ref[pl.ds(base, GROUP), :].astype(F32)
    at = lax.broadcasted_iota(jnp.int32, near.shape, 0) == row % GROUP
    return jnp.sum(jnp.where(at, near, 0.0), axis=0, keepdims=True)


def lane_to_rows(root):
    return jnp.broadcast_to(root, (root.shape[1], root.shape[1])).T


def roots_of(degree_ref, index):
    return lax.rsqrt(degree_ref[pl.ds(index, 1), :].astype(F32))


def factor_block(degree_ref, index):
    return lane_to_rows(roots_of(degree_ref, index))


def hub_roots(degree_ref, hubs_ref):
    tile = degree_ref.shape[1]
    found = []
    for i in range(hubs_ref.shape[0]):
        roots = roots_of(degree_ref, hubs_ref[i] // tile)
        at = lax.broadcasted_iota(jnp.int32, roots.shape, 1) == hubs_ref[i] % tile
        found.append(jnp.sum(jnp.where(at, roots, 0.0), axis=1, keepdims=True))
    return found


def gather_roots(degree_ref, roots_ref, listed, hubs_ref):
    tile = degree_ref.shape[1]
    rows = [roots_of(degree_ref, index) for index, _ in listed]
    lane = lax.broadcasted_iota(jnp.int32, (1, tile), 1)
    last = jnp.zeros((1, tile), F32)
    for i, root in enumerate(hub_roots(degree_ref, hubs_ref)):
        last = jnp.where(lane == i, jnp.broadcast_to(root, (1, tile)), last)
    roots_ref[...] = jnp.concatenate(rows + [last], axis=0)


def quarters(row_count):
    part = row_count // 4
    return [slice(i, i + part) for i in range(0, row_count, part)]


def slots(blocks_ref, count_ref):
    index = lax.axis_index("dom")
    parity = index % 2
    send_most = blocks_ref.shape[2]
    inner = jnp.logical_and(index > 0, index < lax.axis_size("dom") - 1)
    return [
        (blocks_ref[0, side, slot], jnp.logical_and(slot < count_ref[0, side], real))
        for side, real in ((parity, inner), (1 - parity, True))
        for slot in range(send_most)
    ]


def gather_sent(source_ref, target_ref, listed, hubs_ref):
    tile = (target_ref.shape[0] - GROUP) // len(listed)
    width = source_ref.shape[1]
    for i, (index, live) in enumerate(listed):
        block = source_ref[block_rows(index, tile), :]
        target_ref[i * tile : (i + 1) * tile, :] = jnp.where(live, block, jnp.zeros_like(block))
    rows = [one_row(source_ref, hubs_ref[i]) for i in range(hubs_ref.shape[0])]
    rows.append(jnp.zeros((GROUP - len(rows), width), F32))
    target_ref[len(listed) * tile :, :] = jnp.concatenate(rows, axis=0).astype(target_ref.dtype)


def place_received(from_chip_ref, from_core_ref, gathered_ref, received):
    rim_rows = from_chip_ref.shape[0]
    parity = lax.axis_index("dom") % 2
    received[block_rows(parity, rim_rows), :] = from_chip_ref[...]
    received[block_rows(1 - parity, rim_rows), :] = from_core_ref[...]
    received[2 * rim_rows :, :] = gathered_ref[...]


def spread_rows(rows, spread_ref, spread_hbm, copies):
    spread_ref[...] = jnp.broadcast_to(rows[None], spread_ref.shape)
    return copies.start((spread_ref, spread_hbm))


def prologue_kernel(
    blocks_hbm, count_hbm, hubs_hbm, degree_hbm, features_hbm, embeddings_hbm,
    chip_ref, core_ref, spread_hbm,
    blocks_ref, count_ref, hubs_ref, degree_ref, features_ref, embeddings_ref, spread_ref, sems,
):
    copies = Copies(sems)
    tile = degree_ref.shape[1]
    split = features_ref.shape[1]
    tables = copies.start(
        (blocks_hbm, blocks_ref), (count_hbm, count_ref), (hubs_hbm, hubs_ref), (degree_hbm, degree_ref)
    )
    rows = copies.start((features_hbm, features_ref), (embeddings_hbm, embeddings_ref))
    finish(tables)
    listed = slots(blocks_ref, count_ref)
    factors = [factor_block(degree_ref, index) for index, _ in listed]
    finish(rows)
    hubs = []
    for i, root in enumerate(hub_roots(degree_ref, hubs_ref)):
        row = hubs_ref[i]
        whole = jnp.concatenate([one_row(features_ref, row), one_row(embeddings_ref, row)], axis=1)
        hubs.append(scale_rows(whole, jnp.broadcast_to(root, (1, tile))))
    writes = spread_rows(jnp.concatenate(hubs, axis=0).astype(BF16), spread_ref, spread_hbm, copies)
    half = len(listed) // 2
    for i, (index, live) in enumerate(listed):
        target = (chip_ref, core_ref)[i // half]
        into = slice((i % half) * tile, (i % half + 1) * tile)
        for source, columns in ((features_ref, slice(0, split)), (embeddings_ref, slice(split, None))):
            block = scale_rows(source[block_rows(index, tile), :].astype(F32), factors[i])
            target[into, columns] = jnp.where(live, block, 0.0).astype(BF16)
    finish(writes)


def bulk_kernel(*refs, hop, rim, per_block):
    refs = list(refs)
    take = lambda n: [refs.pop(0) for _ in range(n)]
    blocks_hbm, count_hbm, hubs_hbm, columns_hbm, tiles_hbm = take(5)
    first, last = hop == 0, hop == HOPS - 1
    if first:
        degree_hbm, features_hbm, embeddings_hbm, weight_hbm = take(4)
        own_hbm, own_tail, own_sent, mixed_out, dmat_out, mixed_sent, roots_sent = take(7)
    else:
        old_own_hbm, mixed_hbm, dmat_hbm, received_hbm = take(4)
        if hop > 1:
            take(2)
        (old_tail,) = take(1)
        all_features, all_embeddings, own_hbm = take(3)
        if last:
            mixed_ref, dmat_ref = take(2)
        else:
            own_tail, own_sent = take(2)
    blocks_ref, count_ref, hubs_ref, columns_ref = take(4)
    tiles_ref, z_ref, own_ref, features_ref, embeddings_ref = take(5)
    if not last:
        mixed_ref, dmat_ref = take(2)
    if first:
        degree_ref, weight_ref, sems = refs
    else:
        received, old_own_ref, sems = refs
    copies = Copies(sems)
    blocks, _, tile, _ = tiles_ref.shape
    row_count, width = z_ref.shape
    split = features_ref.shape[1]
    every = [slice(b * tile, (b + 1) * tile) for b in range(blocks)]

    tables = copies.start((columns_hbm, columns_ref))
    if not last:
        tables += copies.start((blocks_hbm, blocks_ref), (count_hbm, count_ref), (hubs_hbm, hubs_ref))
    writes = []
    if first:
        finish(copies.start((degree_hbm, degree_ref), (features_hbm, features_ref),
                            (embeddings_hbm, embeddings_ref)))
        late = copies.start((tiles_hbm, tiles_ref), (weight_hbm, weight_ref))
        for b, rows in enumerate(every):
            dmat = factor_block(degree_ref, b)
            dmat_ref[rows, :] = dmat
            z_ref[rows, :split] = scale_rows(features_ref[rows, :].astype(F32), dmat).astype(BF16)
            z_ref[rows, split:] = scale_rows(embeddings_ref[rows, :].astype(F32), dmat).astype(BF16)
    else:
        inputs = copies.start((received_hbm, received))
        held = old_own_ref.shape[0]
        parts = []
        for rows in every:
            pairs = [(mixed_hbm.at[rows, :], mixed_ref.at[rows, :]), (dmat_hbm.at[rows, :], dmat_ref.at[rows, :])]
            if rows.stop <= held:
                pairs.append((old_own_hbm.at[rows, :], old_own_ref.at[rows, :]))
            parts.append(copies.start(*pairs))
        late = copies.start((tiles_hbm, tiles_ref))
        finish(inputs)
        for b, rows in enumerate(every):
            if b % 4 == 0:
                finish([copy for part in parts[b : b + 4] for copy in part])
            total = jnp.dot(mixed_ref[rows, :], received[...], preferred_element_type=F32)
            dmat = dmat_ref[rows, :]
            old = old_own_ref[rows, :] if rows.stop <= held else old_tail[rows.start - held : rows.stop - held, :]
            fresh = scale_rows(old.astype(F32) + total, dmat).astype(BF16)
            features_ref[rows, :] = fresh[:, :split]
            embeddings_ref[rows, :] = fresh[:, split:]
            z_ref[rows, :] = scale_rows(fresh.astype(F32), dmat).astype(BF16)
        writes += copies.start(
            (features_ref, all_features.at[hop - 1]), (embeddings_ref, all_embeddings.at[hop - 1])
        )
    finish(late + tables)
    for b, rows in enumerate(every):
        columns = [columns_ref[k, b] for k in range(per_block)]
        tiles = [tiles_ref[b, k] for k in range(per_block)]
        values = jnp.concatenate(
            [jnp.where(c < blocks, t, jnp.zeros_like(t)) for c, t in zip(columns, tiles)], axis=1
        )
        picked = jnp.concatenate([z_ref[block_rows(jnp.minimum(c, blocks - 1), tile), :] for c in columns], axis=0)
        own = jnp.dot(values, picked, preferred_element_type=F32).astype(BF16)
        own_ref[rows, :] = own
        if rows.stop <= own_hbm.shape[0]:
            writes += copies.start((own_ref.at[rows, :], own_hbm.at[rows, :]))
        else:
            own_tail[rows.start - own_hbm.shape[0] : rows.stop - own_hbm.shape[0], :] = own
        if first:
            for slot in range(rim):
                total = jnp.zeros((tile, tile), F32)
                for c, t in zip(columns, tiles):
                    total += jnp.where(c == blocks + slot, t, jnp.zeros_like(t)).astype(F32)
                mixed_ref[rows, slot * tile : (slot + 1) * tile] = total.astype(BF16)
            mixed_ref[rows, rim * tile :] = weight_ref[:, rows].astype(F32).T.astype(BF16)
    if first:
        writes += copies.start((mixed_ref, mixed_out), (dmat_ref, dmat_out))
    if not last:
        listed = slots(blocks_ref, count_ref)
        gather_sent(own_ref, own_sent, listed, hubs_ref)
    if first:
        gather_sent(mixed_ref, mixed_sent, listed, hubs_ref)
        gather_roots(degree_ref, roots_sent, listed, hubs_ref)
    finish(writes)


def edge_kernel(
    own_ref, mixed_ref, roots_ref, from_chip_ref, from_core_ref, gathered_ref,
    chip_ref, core_ref, spread_hbm, received_hbm,
    received, spread_ref, sems,
):
    copies = Copies(sems)
    rim_rows = chip_ref.shape[0]
    hub_dev = spread_ref.shape[1]
    place_received(from_chip_ref, from_core_ref, gathered_ref, received)
    writes = copies.start((received, received_hbm))
    tile = roots_ref.shape[1]

    def fresh(part):
        rows = slice(part * tile, min((part + 1) * tile, own_ref.shape[0]))
        total = jnp.dot(mixed_ref[rows, :], received[...], preferred_element_type=F32)
        dmat = lane_to_rows(roots_ref[part : part + 1, :])[: rows.stop - rows.start]
        kept = scale_rows(own_ref[rows, :].astype(F32) + total, dmat).astype(BF16)
        return scale_rows(kept.astype(F32), dmat).astype(BF16)

    send_most = rim_rows // tile
    hub = fresh(2 * send_most)
    writes += spread_rows(hub[:hub_dev], spread_ref, spread_hbm, copies)
    for slot in range(send_most):
        chip_ref[slot * tile : (slot + 1) * tile, :] = fresh(slot)
        core_ref[slot * tile : (slot + 1) * tile, :] = fresh(send_most + slot)
    finish(writes)


def final_kernel(
    own_hbm, mixed_ref, dmat_ref, from_chip_ref, from_core_ref, gathered_ref, _, __,
    all_features, all_embeddings,
    own_ref, total_ref, features_ref, embeddings_ref, received, sems,
):
    copies = Copies(sems)
    split = features_ref.shape[1]
    row_count = own_ref.shape[0]
    half = row_count // 2
    reads = [
        copies.start((own_hbm.at[rows, :], own_ref.at[rows, :]))
        for rows in (slice(0, half), slice(half, row_count))
    ]
    place_received(from_chip_ref, from_core_ref, gathered_ref, received)
    tile = dmat_ref.shape[1]
    parts = [slice(at, at + tile) for at in range(0, row_count, tile)]
    ahead = len(parts) // 2
    for rows in parts[:ahead]:
        total_ref[rows, :] = jnp.dot(mixed_ref[rows, :], received[...], preferred_element_type=F32)
    finish(reads[0])
    writes = []
    for i, rows in enumerate(parts):
        if i == ahead:
            finish(reads[1])
        if i < ahead:
            total = total_ref[rows, :]
        else:
            total = jnp.dot(mixed_ref[rows, :], received[...], preferred_element_type=F32)
        fresh = scale_rows(own_ref[rows, :].astype(F32) + total, dmat_ref[rows, :]).astype(BF16)
        features_ref[rows, :] = fresh[:, :split]
        embeddings_ref[rows, :] = fresh[:, split:]
        writes += copies.start(
            (features_ref.at[rows, :], all_features.at[HOPS - 1, rows, :]),
            (embeddings_ref.at[rows, :], all_embeddings.at[HOPS - 1, rows, :]),
        )
    finish(writes)


def body(
    features, embeddings, tile_values, tile_columns, send_blocks, send_count, hub_rows, hub_weight, degree,
):
    row_count, split = features.shape
    blocks, per_block, tile, _ = tile_values.shape
    extra = embeddings.shape[1]
    width = split + extra
    send_most = send_blocks.shape[2]
    hub_dev = hub_rows.shape[0]
    hub_total = hub_weight.shape[1]
    count = lax.axis_size("dom")
    rim = 2 * send_most
    deep = rim * tile + hub_total
    sent = rim * tile + GROUP

    vmem = pl.BlockSpec(memory_space=VMEM)
    hbm = pl.BlockSpec(memory_space=pltpu.HBM)
    shape = jax.ShapeDtypeStruct
    int32 = jnp.int32

    def pin(*values):
        return [pltpu.with_memory_space_constraint(value, pltpu.HBM) for value in values]

    def call(kernel, name, flops, out_shape, scratch, sems, in_hbm, operands, aliases={}):
        specs = [hbm] * in_hbm + [vmem] * (len(operands) - in_hbm)
        for source, target in aliases.items():
            if not isinstance(out_shape[target], shape):
                specs[source] = hbm
        return pl.pallas_call(
            kernel,
            name=name,
            out_shape=out_shape,
            in_specs=specs,
            out_specs=[vmem if isinstance(out, shape) else hbm for out in out_shape],
            scratch_shapes=scratch + [pltpu.SemaphoreType.DMA((sems,))],
            input_output_aliases=aliases,
            compiler_params=pltpu.CompilerParams(vmem_limit_bytes=32 * 2**20),
            cost_estimate=pl.CostEstimate(flops=flops, bytes_accessed=0, transcendentals=0),
        )(*operands)

    tables = [SMEM(send_blocks.shape, int32), SMEM(send_count.shape, int32), SMEM(hub_rows.shape, int32)]
    sends = [
        shape((send_most * tile, width), BF16), shape((send_most * tile, width), BF16),
        pltpu.HBM((count, hub_dev, width), BF16),
    ]
    spread_buffer = VMEM((count, hub_dev, width), BF16)
    whole = [pltpu.HBM((HOPS, row_count, split), BF16), pltpu.HBM((HOPS, row_count, extra), BF16)]
    row_buffers = [VMEM((row_count, split), BF16), VMEM((row_count, extra), BF16)]
    lists = pin(send_blocks, send_count, hub_rows)
    rows = pin(degree.reshape(blocks, tile), features, embeddings)
    to_chip, to_core, spread = call(
        prologue_kernel, "prologue", 10**8, sends,
        tables + [VMEM((blocks, tile), int32)] + row_buffers + [spread_buffer], 7, 6, lists + rows,
    )

    core_pairs = [(i, i ^ 1) for i in range(count) if i ^ 1 < count]
    chip_pairs = [p for i in range(1, count, 2) for p in ((i, (i + 1) % count), ((i + 1) % count, i))]
    fixed = lists + pin(tile_columns.T, tile_values)
    out = []
    for hop in range(HOPS):
        first, last = hop == 0, hop == HOPS - 1
        from_chip = lax.ppermute(to_chip, "dom", chip_pairs)
        from_core = lax.ppermute(to_core, "dom", core_pairs)
        gathered = lax.all_to_all(spread, "dom", 0, 0).reshape(hub_total, width)

        scratch = tables + [
            SMEM((per_block, blocks), int32), VMEM(tile_values.shape, BF16), VMEM((row_count, width), BF16),
            VMEM((row_count, width), BF16),
        ] + row_buffers
        if not last:
            scratch += [VMEM((row_count, deep), BF16), VMEM((row_count, tile), F32)]
        aliases = {}
        tail = 0 if last else KEPT * tile
        full_own = pltpu.HBM((row_count - tail, width), BF16)
        sent_shapes = [shape((tail, width), BF16), shape((sent, width), BF16), shape((sent, deep), BF16)]
        if first:
            operands = fixed + rows + pin(hub_weight.T)
            out_shape = [full_own] + sent_shapes + [shape((rim + 1, tile), F32)]
            out_shape[3:3] = [pltpu.HBM((row_count, deep), BF16), pltpu.HBM((row_count, tile), F32)]
            scratch += [VMEM((blocks, tile), int32), VMEM((hub_total, row_count), BF16)]
        else:
            operands = fixed + pin(own, mixed, dmat, received)
            if out:
                aliases = {len(operands): 0, len(operands) + 1: 1}
                operands += pin(*out)
            operands += [own_tail]
            out_shape = whole + [full_own]
            out_shape += [shape((row_count, deep), BF16), shape((row_count, tile), F32)] if last else sent_shapes[:2]
            scratch += [VMEM((deep, width), BF16), VMEM((row_count - KEPT * tile, width), BF16)]
        got = call(
            functools.partial(bulk_kernel, hop=hop, rim=rim, per_block=per_block), f"bulk{hop}",
            4 * row_count * per_block * tile * width, out_shape, scratch, 12 + 4 * blocks,
            len(operands) - (not first), operands, aliases,
        )
        if first:
            own, own_tail, own_sent, mixed, dmat, mixed_sent, roots_sent = got
        else:
            out, (own, *got) = got[:2], got[2:]
            if last:
                mixed_here, dmat_here = got
            else:
                own_tail, own_sent = got

        flops = 2 * row_count * deep * width
        if last:
            operands = pin(own) + [mixed_here, dmat_here, from_chip, from_core, gathered]
            aliases = {len(operands): 0, len(operands) + 1: 1}
            out = call(
                final_kernel, "final", flops, whole,
                [VMEM((row_count, width), BF16), VMEM((row_count, width), F32)] + row_buffers
                + [VMEM((deep, width), BF16)], 2 + 2 * blocks,
                1, operands + pin(*out), aliases,
            )
        else:
            to_chip, to_core, spread, received = call(
                edge_kernel, f"edge{hop}", flops, sends + [pltpu.HBM((deep, width), BF16)],
                [VMEM((deep, width), BF16), spread_buffer], 2,
                0, [own_sent, mixed_sent, roots_sent, from_chip, from_core, gathered],
                {3: 0, 4: 1},
            )
    return out[0], out[1]


def solution(mesh):
    placed = (
        P("dom", None),
        P("dom", None),
        P("dom", None, None, None),
        P("dom", None),
        P("dom", None, None),
        P("dom", None),
        P("dom"),
        P("dom", None),
        P("dom"),
    )
    return jax.shard_map(
        body,
        mesh=mesh,
        in_specs=placed,
        out_specs=(P(None, "dom", None), P(None, "dom", None)),
        check_vma=False,
    )
```

```python
import functools

import jax
import jax.numpy as jnp
from jax import lax
from jax.experimental import pallas as pl
from jax.experimental.pallas import tpu as pltpu
from jax.sharding import PartitionSpec as P

HOPS = 3
VMEM = pltpu.VMEM
SMEM = pltpu.SMEM
BF16 = jnp.bfloat16
F32 = jnp.float32
GROUP = 16
KEPT = 2


def scale_rows(value, dmat):
    lanes = dmat.shape[1]
    pieces = [value[:, i : i + lanes] * dmat for i in range(0, value.shape[1], lanes)]
    return pieces[0] if len(pieces) == 1 else jnp.concatenate(pieces, axis=1)


def finish(copies):
    for copy in copies:
        copy.wait()


class Copies:
    def __init__(self, sems):
        self.sems, self.used = sems, 0

    def start(self, *pairs):
        begun = []
        for source, target in pairs:
            copy = pltpu.make_async_copy(source, target, self.sems.at[self.used])
            copy.start()
            begun.append(copy)
            self.used += 1
        return begun


def block_rows(index, tile):
    return pl.ds(pl.multiple_of(index * tile, tile), tile)


def one_row(ref, row):
    base = pl.multiple_of(row // GROUP * GROUP, GROUP)
    near = ref[pl.ds(base, GROUP), :].astype(F32)
    at = lax.broadcasted_iota(jnp.int32, near.shape, 0) == row % GROUP
    return jnp.sum(jnp.where(at, near, 0.0), axis=0, keepdims=True)


def lane_to_rows(root):
    return jnp.broadcast_to(root, (root.shape[1], root.shape[1])).T


def roots_of(degree_ref, index):
    return lax.rsqrt(degree_ref[pl.ds(index, 1), :].astype(F32))


def factor_block(degree_ref, index):
    return lane_to_rows(roots_of(degree_ref, index))


def hub_roots(degree_ref, hubs_ref):
    tile = degree_ref.shape[1]
    found = []
    for i in range(hubs_ref.shape[0]):
        roots = roots_of(degree_ref, hubs_ref[i] // tile)
        at = lax.broadcasted_iota(jnp.int32, roots.shape, 1) == hubs_ref[i] % tile
        found.append(jnp.sum(jnp.where(at, roots, 0.0), axis=1, keepdims=True))
    return found


def gather_roots(degree_ref, roots_ref, listed, hubs_ref):
    tile = degree_ref.shape[1]
    rows = [roots_of(degree_ref, index) for index, _ in listed]
    lane = lax.broadcasted_iota(jnp.int32, (1, tile), 1)
    last = jnp.zeros((1, tile), F32)
    for i, root in enumerate(hub_roots(degree_ref, hubs_ref)):
        last = jnp.where(lane == i, jnp.broadcast_to(root, (1, tile)), last)
    roots_ref[...] = jnp.concatenate(rows + [last], axis=0)


def quarters(row_count):
    part = row_count // 4
    return [slice(i, i + part) for i in range(0, row_count, part)]


def slots(blocks_ref, count_ref):
    index = lax.axis_index("dom")
    parity = index % 2
    send_most = blocks_ref.shape[2]
    inner = jnp.logical_and(index > 0, index < lax.axis_size("dom") - 1)
    return [
        (blocks_ref[0, side, slot], jnp.logical_and(slot < count_ref[0, side], real))
        for side, real in ((parity, inner), (1 - parity, True))
        for slot in range(send_most)
    ]


def gather_sent(source_ref, target_ref, listed, hubs_ref):
    tile = (target_ref.shape[0] - GROUP) // len(listed)
    width = source_ref.shape[1]
    for i, (index, live) in enumerate(listed):
        block = source_ref[block_rows(index, tile), :]
        target_ref[i * tile : (i + 1) * tile, :] = jnp.where(live, block, jnp.zeros_like(block))
    rows = [one_row(source_ref, hubs_ref[i]) for i in range(hubs_ref.shape[0])]
    rows.append(jnp.zeros((GROUP - len(rows), width), F32))
    target_ref[len(listed) * tile :, :] = jnp.concatenate(rows, axis=0).astype(target_ref.dtype)


def place_received(from_chip_ref, from_core_ref, gathered_ref, received):
    rim_rows = from_chip_ref.shape[0]
    parity = lax.axis_index("dom") % 2
    received[block_rows(parity, rim_rows), :] = from_chip_ref[...]
    received[block_rows(1 - parity, rim_rows), :] = from_core_ref[...]
    received[2 * rim_rows :, :] = gathered_ref[...]


def spread_rows(rows, spread_ref, spread_hbm, copies):
    spread_ref[...] = jnp.broadcast_to(rows[None], spread_ref.shape)
    return copies.start((spread_ref, spread_hbm))


def prologue_kernel(
    blocks_hbm, count_hbm, hubs_hbm, degree_hbm, features_hbm, embeddings_hbm,
    chip_ref, core_ref, spread_hbm,
    blocks_ref, count_ref, hubs_ref, degree_ref, features_ref, embeddings_ref, spread_ref, sems,
):
    copies = Copies(sems)
    tile = degree_ref.shape[1]
    split = features_ref.shape[1]
    tables = copies.start(
        (blocks_hbm, blocks_ref), (count_hbm, count_ref), (hubs_hbm, hubs_ref), (degree_hbm, degree_ref)
    )
    rows = copies.start((features_hbm, features_ref), (embeddings_hbm, embeddings_ref))
    finish(tables)
    listed = slots(blocks_ref, count_ref)
    factors = [factor_block(degree_ref, index) for index, _ in listed]
    hub_factors = [jnp.broadcast_to(root, (1, tile)) for root in hub_roots(degree_ref, hubs_ref)]
    finish(rows)
    hubs = []
    for i, factor in enumerate(hub_factors):
        row = hubs_ref[i]
        whole = jnp.concatenate([one_row(features_ref, row), one_row(embeddings_ref, row)], axis=1)
        hubs.append(scale_rows(whole, factor))
    writes = spread_rows(jnp.concatenate(hubs, axis=0).astype(BF16), spread_ref, spread_hbm, copies)
    half = len(listed) // 2
    for i, (index, live) in enumerate(listed):
        target = (chip_ref, core_ref)[i // half]
        into = slice((i % half) * tile, (i % half + 1) * tile)
        for source, columns in ((features_ref, slice(0, split)), (embeddings_ref, slice(split, None))):
            block = scale_rows(source[block_rows(index, tile), :].astype(F32), factors[i])
            target[into, columns] = jnp.where(live, block, 0.0).astype(BF16)
    finish(writes)


def bulk_kernel(*refs, hop, rim, per_block):
    refs = list(refs)
    take = lambda n: [refs.pop(0) for _ in range(n)]
    blocks_hbm, count_hbm, hubs_hbm, columns_hbm, tiles_hbm = take(5)
    first, last = hop == 0, hop == HOPS - 1
    if first:
        degree_hbm, features_hbm, embeddings_hbm, weight_hbm = take(4)
        own_hbm, own_tail, own_sent, mixed_out, dmat_out, mixed_sent, roots_sent = take(7)
    else:
        old_own_hbm, mixed_hbm, dmat_hbm, received_hbm = take(4)
        if hop > 1:
            take(2)
        (old_tail,) = take(1)
        all_features, all_embeddings, own_hbm = take(3)
        if last:
            mixed_ref, dmat_ref = take(2)
        else:
            own_tail, own_sent = take(2)
    blocks_ref, count_ref, hubs_ref, columns_ref = take(4)
    tiles_ref, z_ref, own_ref, features_ref, embeddings_ref = take(5)
    if not last:
        mixed_ref, dmat_ref = take(2)
    if first:
        degree_ref, weight_ref, sems = refs
    else:
        received, old_own_ref, sems = refs
    copies = Copies(sems)
    blocks, _, tile, _ = tiles_ref.shape
    row_count, width = z_ref.shape
    split = features_ref.shape[1]
    every = [slice(b * tile, (b + 1) * tile) for b in range(blocks)]

    tables = copies.start((columns_hbm, columns_ref))
    if not last:
        tables += copies.start((blocks_hbm, blocks_ref), (count_hbm, count_ref), (hubs_hbm, hubs_ref))
    writes = []
    if first:
        finish(copies.start((degree_hbm, degree_ref), (features_hbm, features_ref),
                            (embeddings_hbm, embeddings_ref)))
        late = copies.start((tiles_hbm, tiles_ref), (weight_hbm, weight_ref))
        for b, rows in enumerate(every):
            dmat = factor_block(degree_ref, b)
            dmat_ref[rows, :] = dmat
            z_ref[rows, :split] = scale_rows(features_ref[rows, :].astype(F32), dmat).astype(BF16)
            z_ref[rows, split:] = scale_rows(embeddings_ref[rows, :].astype(F32), dmat).astype(BF16)
    else:
        inputs = copies.start((received_hbm, received))
        held = old_own_ref.shape[0]
        parts = []
        for rows in every:
            pairs = [(mixed_hbm.at[rows, :], mixed_ref.at[rows, :]), (dmat_hbm.at[rows, :], dmat_ref.at[rows, :])]
            if rows.stop <= held:
                pairs.append((old_own_hbm.at[rows, :], old_own_ref.at[rows, :]))
            parts.append(copies.start(*pairs))
        late = copies.start((tiles_hbm, tiles_ref))
        finish(inputs)
        for b, rows in enumerate(every):
            if b % 4 == 0:
                finish([copy for part in parts[b : b + 4] for copy in part])
            total = jnp.dot(mixed_ref[rows, :], received[...], preferred_element_type=F32)
            dmat = dmat_ref[rows, :]
            old = old_own_ref[rows, :] if rows.stop <= held else old_tail[rows.start - held : rows.stop - held, :]
            fresh = scale_rows(old.astype(F32) + total, dmat).astype(BF16)
            features_ref[rows, :] = fresh[:, :split]
            embeddings_ref[rows, :] = fresh[:, split:]
            z_ref[rows, :] = scale_rows(fresh.astype(F32), dmat).astype(BF16)
        writes += copies.start(
            (features_ref, all_features.at[hop - 1]), (embeddings_ref, all_embeddings.at[hop - 1])
        )
    finish(late + tables)
    for b, rows in enumerate(every):
        columns = [columns_ref[k, b] for k in range(per_block)]
        tiles = [tiles_ref[b, k] for k in range(per_block)]
        values = jnp.concatenate(
            [jnp.where(c < blocks, t, jnp.zeros_like(t)) for c, t in zip(columns, tiles)], axis=1
        )
        picked = jnp.concatenate([z_ref[block_rows(jnp.minimum(c, blocks - 1), tile), :] for c in columns], axis=0)
        own = jnp.dot(values, picked, preferred_element_type=F32).astype(BF16)
        own_ref[rows, :] = own
        if rows.stop <= own_hbm.shape[0]:
            writes += copies.start((own_ref.at[rows, :], own_hbm.at[rows, :]))
        else:
            own_tail[rows.start - own_hbm.shape[0] : rows.stop - own_hbm.shape[0], :] = own
        if first:
            for slot in range(rim):
                total = jnp.zeros((tile, tile), F32)
                for c, t in zip(columns, tiles):
                    total += jnp.where(c == blocks + slot, t, jnp.zeros_like(t)).astype(F32)
                mixed_ref[rows, slot * tile : (slot + 1) * tile] = total.astype(BF16)
            mixed_ref[rows, rim * tile :] = weight_ref[:, rows].astype(F32).T.astype(BF16)
    if first:
        writes += copies.start((mixed_ref, mixed_out), (dmat_ref, dmat_out))
    if not last:
        listed = slots(blocks_ref, count_ref)
        gather_sent(own_ref, own_sent, listed, hubs_ref)
    if first:
        gather_sent(mixed_ref, mixed_sent, listed, hubs_ref)
        gather_roots(degree_ref, roots_sent, listed, hubs_ref)
    finish(writes)


def edge_kernel(
    own_ref, mixed_ref, roots_ref, from_chip_ref, from_core_ref, gathered_ref,
    chip_ref, core_ref, spread_hbm, received_hbm,
    received, spread_ref, sems,
):
    copies = Copies(sems)
    rim_rows = chip_ref.shape[0]
    hub_dev = spread_ref.shape[1]
    place_received(from_chip_ref, from_core_ref, gathered_ref, received)
    writes = copies.start((received, received_hbm))
    tile = roots_ref.shape[1]

    def fresh(part):
        rows = slice(part * tile, min((part + 1) * tile, own_ref.shape[0]))
        total = jnp.dot(mixed_ref[rows, :], received[...], preferred_element_type=F32)
        dmat = lane_to_rows(roots_ref[part : part + 1, :])[: rows.stop - rows.start]
        kept = scale_rows(own_ref[rows, :].astype(F32) + total, dmat).astype(BF16)
        return scale_rows(kept.astype(F32), dmat).astype(BF16)

    send_most = rim_rows // tile
    hub = fresh(2 * send_most)
    writes += spread_rows(hub[:hub_dev], spread_ref, spread_hbm, copies)
    for slot in range(send_most):
        chip_ref[slot * tile : (slot + 1) * tile, :] = fresh(slot)
        core_ref[slot * tile : (slot + 1) * tile, :] = fresh(send_most + slot)
    finish(writes)


def final_kernel(
    own_hbm, mixed_ref, dmat_ref, from_chip_ref, from_core_ref, gathered_ref, _, __,
    all_features, all_embeddings,
    own_ref, total_ref, features_ref, embeddings_ref, received, sems,
):
    copies = Copies(sems)
    split = features_ref.shape[1]
    row_count = own_ref.shape[0]
    half = row_count // 2
    reads = [
        copies.start((own_hbm.at[rows, :], own_ref.at[rows, :]))
        for rows in (slice(0, half), slice(half, row_count))
    ]
    place_received(from_chip_ref, from_core_ref, gathered_ref, received)
    tile = dmat_ref.shape[1]
    parts = [slice(at, at + tile) for at in range(0, row_count, tile)]
    ahead = len(parts) // 2
    for rows in parts[:ahead]:
        total_ref[rows, :] = jnp.dot(mixed_ref[rows, :], received[...], preferred_element_type=F32)
    finish(reads[0])
    writes = []
    for i, rows in enumerate(parts):
        if i == ahead:
            finish(reads[1])
        if i < ahead:
            total = total_ref[rows, :]
        else:
            total = jnp.dot(mixed_ref[rows, :], received[...], preferred_element_type=F32)
        fresh = scale_rows(own_ref[rows, :].astype(F32) + total, dmat_ref[rows, :]).astype(BF16)
        features_ref[rows, :] = fresh[:, :split]
        embeddings_ref[rows, :] = fresh[:, split:]
        writes += copies.start(
            (features_ref.at[rows, :], all_features.at[HOPS - 1, rows, :]),
            (embeddings_ref.at[rows, :], all_embeddings.at[HOPS - 1, rows, :]),
        )
    finish(writes)


def body(
    features, embeddings, tile_values, tile_columns, send_blocks, send_count, hub_rows, hub_weight, degree,
):
    row_count, split = features.shape
    blocks, per_block, tile, _ = tile_values.shape
    extra = embeddings.shape[1]
    width = split + extra
    send_most = send_blocks.shape[2]
    hub_dev = hub_rows.shape[0]
    hub_total = hub_weight.shape[1]
    count = lax.axis_size("dom")
    rim = 2 * send_most
    deep = rim * tile + hub_total
    sent = rim * tile + GROUP

    vmem = pl.BlockSpec(memory_space=VMEM)
    hbm = pl.BlockSpec(memory_space=pltpu.HBM)
    shape = jax.ShapeDtypeStruct
    int32 = jnp.int32

    def pin(*values):
        return [pltpu.with_memory_space_constraint(value, pltpu.HBM) for value in values]

    def call(kernel, name, flops, out_shape, scratch, sems, in_hbm, operands, aliases={}):
        specs = [hbm] * in_hbm + [vmem] * (len(operands) - in_hbm)
        for source, target in aliases.items():
            if not isinstance(out_shape[target], shape):
                specs[source] = hbm
        return pl.pallas_call(
            kernel,
            name=name,
            out_shape=out_shape,
            in_specs=specs,
            out_specs=[vmem if isinstance(out, shape) else hbm for out in out_shape],
            scratch_shapes=scratch + [pltpu.SemaphoreType.DMA((sems,))],
            input_output_aliases=aliases,
            compiler_params=pltpu.CompilerParams(vmem_limit_bytes=32 * 2**20),
            cost_estimate=pl.CostEstimate(flops=flops, bytes_accessed=0, transcendentals=0),
        )(*operands)

    tables = [SMEM(send_blocks.shape, int32), SMEM(send_count.shape, int32), SMEM(hub_rows.shape, int32)]
    sends = [
        shape((send_most * tile, width), BF16), shape((send_most * tile, width), BF16),
        pltpu.HBM((count, hub_dev, width), BF16),
    ]
    spread_buffer = VMEM((count, hub_dev, width), BF16)
    whole = [pltpu.HBM((HOPS, row_count, split), BF16), pltpu.HBM((HOPS, row_count, extra), BF16)]
    row_buffers = [VMEM((row_count, split), BF16), VMEM((row_count, extra), BF16)]
    lists = pin(send_blocks, send_count, hub_rows)
    rows = pin(degree.reshape(blocks, tile), features, embeddings)
    to_chip, to_core, spread = call(
        prologue_kernel, "prologue", 10**8, sends,
        tables + [VMEM((blocks, tile), int32)] + row_buffers + [spread_buffer], 7, 6, lists + rows,
    )

    core_pairs = [(i, i ^ 1) for i in range(count) if i ^ 1 < count]
    chip_pairs = [p for i in range(1, count, 2) for p in ((i, (i + 1) % count), ((i + 1) % count, i))]
    fixed = lists + pin(tile_columns.T, tile_values)
    out = []
    for hop in range(HOPS):
        first, last = hop == 0, hop == HOPS - 1
        from_chip = lax.ppermute(to_chip, "dom", chip_pairs)
        from_core = lax.ppermute(to_core, "dom", core_pairs)
        gathered = lax.all_to_all(spread, "dom", 0, 0).reshape(hub_total, width)

        scratch = tables + [
            SMEM((per_block, blocks), int32), VMEM(tile_values.shape, BF16), VMEM((row_count, width), BF16),
            VMEM((row_count, width), BF16),
        ] + row_buffers
        if not last:
            scratch += [VMEM((row_count, deep), BF16), VMEM((row_count, tile), F32)]
        aliases = {}
        tail = 0 if last else KEPT * tile
        full_own = pltpu.HBM((row_count - tail, width), BF16)
        sent_shapes = [shape((tail, width), BF16), shape((sent, width), BF16), shape((sent, deep), BF16)]
        if first:
            operands = fixed + rows + pin(hub_weight.T)
            out_shape = [full_own] + sent_shapes + [shape((rim + 1, tile), F32)]
            out_shape[3:3] = [pltpu.HBM((row_count, deep), BF16), pltpu.HBM((row_count, tile), F32)]
            scratch += [VMEM((blocks, tile), int32), VMEM((hub_total, row_count), BF16)]
        else:
            operands = fixed + pin(own, mixed, dmat, received)
            if out:
                aliases = {len(operands): 0, len(operands) + 1: 1}
                operands += pin(*out)
            operands += [own_tail]
            out_shape = whole + [full_own]
            out_shape += [shape((row_count, deep), BF16), shape((row_count, tile), F32)] if last else sent_shapes[:2]
            scratch += [VMEM((deep, width), BF16), VMEM((row_count - KEPT * tile, width), BF16)]
        got = call(
            functools.partial(bulk_kernel, hop=hop, rim=rim, per_block=per_block), f"bulk{hop}",
            4 * row_count * per_block * tile * width, out_shape, scratch, 12 + 4 * blocks,
            len(operands) - (not first), operands, aliases,
        )
        if first:
            own, own_tail, own_sent, mixed, dmat, mixed_sent, roots_sent = got
        else:
            out, (own, *got) = got[:2], got[2:]
            if last:
                mixed_here, dmat_here = got
            else:
                own_tail, own_sent = got

        flops = 2 * row_count * deep * width
        if last:
            operands = pin(own) + [mixed_here, dmat_here, from_chip, from_core, gathered]
            aliases = {len(operands): 0, len(operands) + 1: 1}
            out = call(
                final_kernel, "final", flops, whole,
                [VMEM((row_count, width), BF16), VMEM((row_count, width), F32)] + row_buffers
                + [VMEM((deep, width), BF16)], 2 + 2 * blocks,
                1, operands + pin(*out), aliases,
            )
        else:
            to_chip, to_core, spread, received = call(
                edge_kernel, f"edge{hop}", flops, sends + [pltpu.HBM((deep, width), BF16)],
                [VMEM((deep, width), BF16), spread_buffer], 2,
                0, [own_sent, mixed_sent, roots_sent, from_chip, from_core, gathered],
                {3: 0, 4: 1},
            )
    return out[0], out[1]


def solution(mesh):
    placed = (
        P("dom", None),
        P("dom", None),
        P("dom", None, None, None),
        P("dom", None),
        P("dom", None, None),
        P("dom", None),
        P("dom"),
        P("dom", None),
        P("dom"),
    )
    return jax.shard_map(
        body,
        mesh=mesh,
        in_specs=placed,
        out_specs=(P(None, "dom", None), P(None, "dom", None)),
        check_vma=False,
    )
```
